512 devices in a mesh: wide: 64 (over y, z), narrow: 8 (over x, core).
Axes of the slice: x: 4, y: 8, z: 8, core: 2. Of those that a mesh axis runs over, the one named last changes fastest.
Arguments:
- src_field: bfloat16 [2, 16, 1048576], P(None, 'narrow', 'wide'), may hold values from -6 to 6
- src_depth: int32 [1048576], P(('wide', 'narrow')), may hold values from 0 to 16, as said below
- packed_counts: int32 [65536, 64, 128], P(('wide', 'narrow')), may hold values from 0 to 100664832, as said below
- pair_source: int32 [65536], P(('wide', 'narrow')), may hold values from 0 to 15
- pair_home: int32 [65536], P(('wide', 'narrow')), may hold values from 0 to 4095, as said below
- pair_count: int32 [512], P(('wide', 'narrow')), may hold values from 64 to 128, as said below
Outputs:
- remapped: bfloat16 [2, 16, 524288], P(None, 'narrow', 'wide')
The draws below stay inside these ranges and needn't reach their ends.
Inputs may be any that keep to these rules, and one draw needn't show every extreme that they name: `src_depth`: depth 0 marks a dry source cell. `packed_counts`: word (p, i, j) holds count (p, i, j) plus 65536 times count (p, i + 64, j); every count lies between 0 and 1536. The target block pair_home[p] is held by wide index pair_home[p] // 64, which differs by at most 2, counted cyclically over the wide axis, from the wide index of the device that holds pair p. Among the 128 pairs of one device at most 51 have target blocks on one wide index, and on some wide index exactly 51 live pairs of that device. A device's pairs from position pair_count[d] on are padding; some device has all 128 live.
All inputs are finite; a program needn't handle non-finite values.
Results may differ from the reference program's by a relative error of at most 0.0054.
Values may be sent and summed in bfloat16 or wider, within the bound.
A program may use at most 64 MiB of HBM per device.

```python
import jax
import jax.numpy as jnp
from jax import lax

BLK = 128
LEV = 16
VARS = 2
DENOM = 256
REACH = 2
SB_DEV = 16
P_DEV = 128
TB_DEV = 64
CAP = 51
PAIRS = 65536
SRC_CELLS = 1048576
N_WIDE = 64
N_NARROW = 8


def draw_src_depth(key, part):
    key = jax.random.fold_in(key, 404)
    key_land, key_depth = jax.random.split(key)
    blocks = SB_DEV * N_WIDE * N_NARROW
    sea_mask = (jax.random.randint(key_land, (blocks, 1), 0, 5) >= 3).astype(jnp.int32)
    cell_depth = jax.random.randint(key_depth, (blocks, BLK), 1, LEV + 1)
    return (cell_depth * sea_mask).reshape(blocks * BLK).astype(jnp.int32)


def draw_packed_counts(key, part):
    key = jax.random.fold_in(key, 101)
    half_rows = BLK // 2
    key_list = jax.random.split(key, 6)
    array_shape = (P_DEV * N_WIDE * N_NARROW, half_rows, BLK)
    row_ids = jnp.arange(half_rows, dtype=jnp.int32)[:, None]
    column_ids = jnp.arange(BLK, dtype=jnp.int32)[None, :]

    def half_counts(key_spread, key_power, key_factor, offset):
        spread = jax.random.randint(key_spread, array_shape, 0, 4)
        exponent = jax.random.randint(key_power, (array_shape[0], half_rows, 1), 0, 10)
        factor = jax.random.randint(key_factor, (array_shape[0], half_rows, 1), 1, 4)
        diagonal = jnp.power(2, exponent) * factor
        on_diagonal = (column_ids == row_ids + offset)[None, :, :]
        return jnp.where(on_diagonal, diagonal, spread)
    lower_half = half_counts(key_list[0], key_list[1], key_list[2], 0)
    upper_half = half_counts(key_list[3], key_list[4], key_list[5], half_rows)
    return (lower_half + 65536 * upper_half).astype(jnp.int32)


def draw_pair_home(key, part):
    key = jax.random.fold_in(key, 202)
    devices = N_WIDE * N_NARROW
    offset_total = 2 * REACH + 1
    key_rows, key_place = jax.random.split(key)
    head_rows = P_DEV // 2
    slot_ids = jnp.arange(offset_total * CAP, dtype=jnp.int32) // CAP
    wide_of = jnp.arange(devices, dtype=jnp.int32) // N_NARROW

    def one_device(row_key, wide_index):
        key_order, key_head, key_tail = jax.random.split(row_key, 3)
        offset_order = jax.random.permutation(key_order, offset_total).astype(jnp.int32)
        wanted = offset_order[slot_ids][:P_DEV]
        ordering = jnp.concatenate([jax.random.permutation(key_head, head_rows), head_rows + jax.random.permutation(key_tail, P_DEV - head_rows)])
        chosen = wanted[ordering]
        return (wide_index + chosen - REACH + N_WIDE) % N_WIDE
    owners = jax.vmap(one_device)(jax.random.split(key_rows, devices), wide_of)
    local_block = jax.random.randint(key_place, (devices, P_DEV), 0, TB_DEV)
    return (owners * TB_DEV + local_block).reshape(devices * P_DEV).astype(jnp.int32)


def draw_pair_count(key, part):
    key = jax.random.fold_in(key, 303)
    devices = N_WIDE * N_NARROW
    key_counts, key_full = jax.random.split(key)
    counts = jax.random.randint(key_counts, (devices,), P_DEV // 2, P_DEV + 1)
    fullest = jax.random.randint(key_full, (), 0, devices)
    return counts.at[fullest].set(P_DEV).astype(jnp.int32)


def with_ends(result, stream_key, low, high):
    dims = result.shape
    place = [jax.random.randint(jax.random.fold_in(stream_key, axis), (), 0, dims[axis]) for axis in range(len(dims))]
    result = result.at[tuple(place)].set(low)
    longest = dims.index(max(dims))
    place[longest] = (place[longest] + 1) % dims[longest]
    return result.at[tuple(place)].set(high)


def shard_levels(key, extent, cuts, smallest, high):
    def one(position, blocks):
        heights = jax.random.uniform(jax.random.fold_in(jax.random.fold_in(key, 6), position), (blocks,), jnp.float32, smallest / len(cuts), high / len(cuts))
        return jnp.repeat(jnp.exp(heights), extent[position] // blocks).reshape((-1,) + (1,) * (len(extent) - position - 1))

    loudness = one(*cuts[0])
    for cut in cuts[1:]:
        loudness = loudness * one(*cut)
    return loudness


def noise(stream_key, dims, width, most, cuts=(), kind=jnp.bfloat16):
    level = shard_levels(stream_key, dims, cuts, -0.22, 0.18) if cuts else 1.0
    drawn = jax.random.normal(stream_key, dims, jnp.float32) * width * level
    return jnp.minimum(jnp.maximum(drawn, -most), most).astype(kind)


def setup_inputs(seed: int = 0) -> dict:
    streams_of = jax.random.split(jax.random.key(seed), 7)
    src_field = noise(streams_of[0], (VARS, LEV, SRC_CELLS), 1.0, 6.0, ((1, 8), (2, 64)))
    src_depth = draw_src_depth(jax.random.fold_in(streams_of[6], 71), 0)
    packed_counts = draw_packed_counts(jax.random.fold_in(streams_of[6], 71), 0)
    pair_source = with_ends(jax.random.randint(streams_of[3], (PAIRS,), 0, SB_DEV), jax.random.fold_in(streams_of[3], 1), 0, SB_DEV - 1).astype(jnp.int32)
    pair_home = draw_pair_home(jax.random.fold_in(streams_of[6], 71), 0)
    pair_count = draw_pair_count(jax.random.fold_in(streams_of[6], 71), 0)
    return dict(src_field=src_field, src_depth=src_depth, packed_counts=packed_counts, pair_source=pair_source, pair_home=pair_home, pair_count=pair_count)


wet_limit = 1e-3


def unpack_counts(packed_words):
    lower_half = packed_words % 65536
    upper_half = packed_words // 65536
    return jnp.concatenate([lower_half, upper_half], axis=-2)


def stack_cells(field_block, depth_cells):
    level_ids = jnp.arange(field_block.shape[1], dtype=jnp.int32)
    wet_levels = level_ids[:, None] < depth_cells[None, :]
    masked = jnp.where(wet_levels[None, :, :], field_block, jnp.zeros_like(field_block))
    wet_ones = wet_levels.astype(field_block.dtype)
    return jnp.concatenate([jnp.transpose(masked, (1, 0, 2)), wet_ones[:, None, :]], axis=1)


def reference(src_field, src_depth, packed_counts, pair_source, pair_home, pair_count):
    device_total = pair_count.shape[0]
    own_cells = SB_DEV * BLK
    components = VARS + 1
    block_total = jnp.zeros((TB_DEV * N_WIDE, LEV, components, BLK), jnp.float32)

    def add_device(device_index, running):
        device_index = device_index.astype(jnp.int32)
        device_field = lax.dynamic_slice_in_dim(src_field, device_index * own_cells, own_cells, 2)
        cell_depth = lax.dynamic_slice_in_dim(src_depth, device_index * own_cells, own_cells, 0)
        device_packed = lax.dynamic_slice_in_dim(packed_counts, device_index * P_DEV, P_DEV, 0)
        source = lax.dynamic_slice_in_dim(pair_source, device_index * P_DEV, P_DEV, 0)
        home_block = lax.dynamic_slice_in_dim(pair_home, device_index * P_DEV, P_DEV, 0)
        live_count = lax.dynamic_slice_in_dim(pair_count, device_index, 1, 0)[0]
        stacked = stack_cells(device_field, cell_depth).reshape(LEV, components, SB_DEV, BLK)
        picked = jnp.take(stacked, source, axis=2)
        weight = (unpack_counts(device_packed).astype(jnp.float32) / DENOM).astype(jnp.bfloat16)
        pair_terms = jnp.einsum("pts,lcps->plct", weight.astype(jnp.float32), picked.astype(jnp.float32))
        pair_terms = lax.optimization_barrier(pair_terms.astype(jnp.bfloat16)).astype(jnp.float32)
        is_live = jnp.arange(P_DEV, dtype=jnp.int32) < live_count
        pair_terms = jnp.where(is_live[:, None, None, None], pair_terms, jnp.zeros_like(pair_terms))
        return running.at[home_block].add(pair_terms)

    block_total = lax.fori_loop(0, device_total, add_device, block_total)
    numerators = block_total[:, :, :VARS, :]
    wet_total = block_total[:, :, VARS, :]
    covered = wet_total > wet_limit
    safe_wet = jnp.where(covered, wet_total, jnp.ones_like(wet_total))
    remapped = jnp.where(covered[:, :, None, :], numerators / safe_wet[:, :, None, :], jnp.zeros_like(numerators))
    remapped = jnp.transpose(remapped, (2, 1, 0, 3)).reshape(VARS, LEV, TB_DEV * N_WIDE * BLK)
    return remapped.astype(jnp.bfloat16)
```

```python
import functools

import jax
import jax.numpy as jnp
from jax import lax
from jax.experimental import pallas as pl
from jax.experimental.pallas import tpu as pltpu
from jax.sharding import PartitionSpec as P

DENOM = 256
REACH = 2
TB_DEV = 64
WET_LIMIT = 0.001
BATCH = 32
PITCH = 40
MESH = pl.DeviceIdType.MESH


def kernel(
    wide,
    narrow,
    field_in,
    depth_in,
    counts_in,
    source_in,
    home_in,
    live_in,
    out_ref,
    field_v,
    depth_v,
    counts_v,
    home_v,
    source_s,
    live_s,
    target_v,
    target_r,
    field_r,
    rows_f,
    tiles,
    spread,
    terms,
    terms_r,
    select,
    sums,
    own,
    sums_r,
    local_sem,
    counts_sem,
    self_sem,
    field_ss,
    field_rs,
    target_ss,
    target_rs,
    early_ss,
    early_rs,
    early_own,
    late_ss,
    late_rs,
    late_own,
    wide_ss,
    wide_rs,
):
    w = lax.axis_index("wide")
    n = lax.axis_index("narrow")
    pairs, half, lanes = counts_v.shape
    batches = pairs // BATCH
    own_tiles = tiles.shape[0]
    own_cells = own_tiles * lanes
    variables, part = field_v.shape[0], field_v.shape[1]
    levels = narrow * part
    comps = variables + 1
    offsets = 2 * REACH + 1
    shifts = [o for o in range(offsets) if o != REACH]

    def on_narrow(step):
        return lax.rem(n + step, narrow)

    def on_wide(shift):
        return lax.rem(w + shift + wide, wide)

    first = [
        pltpu.make_async_copy(field_in, field_v, local_sem.at[0]),
        pltpu.make_async_copy(home_in, home_v, local_sem.at[1]),
        pltpu.make_async_copy(live_in, live_s, local_sem.at[2]),
        pltpu.make_async_copy(depth_in, depth_v, local_sem.at[3]),
        pltpu.make_async_copy(source_in, source_s, local_sem.at[4]),
    ]
    for copy in first:
        copy.start()

    def counts_copy(b):
        rows = pl.ds(b * BATCH, BATCH)
        return pltpu.make_async_copy(counts_in.at[rows], counts_v.at[rows], counts_sem.at[b])

    for b in range(batches):
        counts_copy(b).start()

    barrier = pltpu.get_barrier_semaphore()
    for step in range(1, narrow):
        pl.semaphore_signal(barrier, inc=1, device_id={"narrow": on_narrow(step)}, device_id_type=MESH)
    for o in shifts:
        pl.semaphore_signal(barrier, inc=1, device_id={"wide": on_wide(o - REACH)}, device_id_type=MESH)

    first[1].wait()
    first[2].wait()
    home = home_v[...]
    slot = lax.broadcasted_iota(jnp.int32, home.shape, 1)
    offset = lax.rem(home // TB_DEV - w + REACH + wide, wide)
    target = jnp.where(slot < live_s[0], offset * TB_DEV + lax.rem(home, TB_DEV), -1)
    target_v[0] = target
    target_r[n] = target
    first[0].wait()
    pl.semaphore_wait(barrier, narrow - 1 + len(shifts))

    order = [2, 6, 4, 3, 7, 5, 1]
    field_out = []
    target_out = []
    for step in order:
        peer = on_narrow(step)
        cells = pl.ds(pl.multiple_of(peer * own_cells, own_cells), own_cells)
        field_out.append(
            pltpu.make_async_remote_copy(
                src_ref=field_v.at[:, :, cells],
                dst_ref=field_r.at[n],
                send_sem=field_ss.at[step],
                recv_sem=field_rs.at[n],
                device_id={"narrow": peer},
                device_id_type=MESH,
            )
        )
        field_out[-1].start()
    for step in order:
        target_out.append(
            pltpu.make_async_remote_copy(
                src_ref=target_v,
                dst_ref=target_r.at[pl.ds(n, 1)],
                send_sem=target_ss.at[step],
                recv_sem=target_rs.at[n],
                device_id={"narrow": on_narrow(step)},
                device_id_type=MESH,
            )
        )
        target_out[-1].start()
    own_span = pl.ds(pl.multiple_of(n * own_cells, own_cells), own_cells)
    own_field = pltpu.make_async_copy(field_v.at[:, :, own_span], field_r.at[n], self_sem)
    own_field.start()

    def field_from(peer):
        return pltpu.make_async_remote_copy(
            src_ref=field_r.at[peer],
            dst_ref=field_r.at[peer],
            send_sem=field_ss.at[0],
            recv_sem=field_rs.at[peer],
            device_id={"narrow": peer},
            device_id_type=MESH,
        )

    own_field.wait()
    for step in range(1, narrow):
        field_from(on_narrow(step)).wait_recv()
    for m in range(narrow):
        for v in range(variables):
            for s in range(own_tiles):
                piece = field_r[m, v, :, s * lanes : (s + 1) * lanes]
                rows_f[s, v * levels + m * part : v * levels + (m + 1) * part, :] = piece.astype(jnp.float32)
    first[3].wait()
    first[4].wait()
    level_ids = lax.broadcasted_iota(jnp.int32, (levels, lanes), 0)
    for s in range(own_tiles):
        wet = level_ids < depth_v[s : s + 1, :]
        tiles[s, :levels, :] = jnp.where(wet, 1.0, 0.0).astype(jnp.bfloat16)
        for v in range(variables):
            rows = rows_f[s, v * levels : (v + 1) * levels, :]
            tiles[s, (v + 1) * levels : (v + 2) * levels, :] = jnp.where(wet, rows, 0.0).astype(jnp.bfloat16)

    def term_copy(b, step, peer, to):
        rows = pl.ds(pl.multiple_of(b * BATCH, BATCH), BATCH)
        return pltpu.make_async_remote_copy(
            src_ref=terms.at[peer, : comps - 1, :, rows],
            dst_ref=terms_r.at[to, : comps - 1, :, rows],
            send_sem=early_ss.at[b, step],
            recv_sem=early_rs.at[b, to],
            device_id={"narrow": peer},
            device_id_type=MESH,
        )

    def own_copy(b):
        rows = pl.ds(pl.multiple_of(b * BATCH, BATCH), BATCH)
        return pltpu.make_async_copy(
            terms.at[n, : comps - 1, :, rows], terms_r.at[n, : comps - 1, :, rows], early_own.at[b]
        )

    def one_batch(b, carry):
        counts_copy(b).wait()

        def one_pair(i, carry):
            p = b * BATCH + i
            words = counts_v[p]
            low = (words & 65535).astype(jnp.float32) * (1.0 / DENOM)
            high = lax.shift_right_logical(words, 16).astype(jnp.float32) * (1.0 / DENOM)
            weight = jnp.concatenate([low.astype(jnp.bfloat16), high.astype(jnp.bfloat16)], axis=0)
            picked = tiles[source_s[p]]
            term = lax.dot_general(
                picked, weight, (((1,), (1,)), ((), ())), preferred_element_type=jnp.float32
            )
            spread[pl.ds(i, comps * levels, stride=PITCH), :] = term
            return carry

        lax.fori_loop(0, BATCH, one_pair, 0, unroll=8)
        rows = pl.ds(pl.multiple_of(b * BATCH, BATCH), BATCH)
        for c in range(comps):
            for l in range(levels):
                r = c * levels + l
                block = spread[r * PITCH : r * PITCH + BATCH, :].astype(jnp.bfloat16)
                terms[l // part, c, l % part, rows, :] = block
        for step in order:
            term_copy(b, step, on_narrow(step), n).start()
        own_copy(b).start()
        return carry

    lax.fori_loop(0, batches, one_batch, 0)

    def late_copy(step, peer, to):
        return pltpu.make_async_remote_copy(
            src_ref=terms.at[peer, comps - 1],
            dst_ref=terms_r.at[to, comps - 1],
            send_sem=late_ss.at[step],
            recv_sem=late_rs.at[to],
            device_id={"narrow": peer},
            device_id_type=MESH,
        )

    for step in order:
        late_copy(step, on_narrow(step), n).start()
    own_late = pltpu.make_async_copy(terms.at[n, comps - 1], terms_r.at[n, comps - 1], late_own)
    own_late.start()

    for step in range(1, narrow):
        peer = on_narrow(step)
        pltpu.make_async_remote_copy(
            src_ref=target_v,
            dst_ref=target_r.at[pl.ds(peer, 1)],
            send_sem=target_ss.at[0],
            recv_sem=target_rs.at[peer],
            device_id={"narrow": peer},
            device_id_type=MESH,
        ).wait_recv()
    for m in range(narrow):
        for o in range(offsets):
            ids = o * TB_DEV + lax.broadcasted_iota(jnp.int32, (TB_DEV, pairs), 0)
            hit = ids == target_r[m]
            select[o, :, m * pairs : (m + 1) * pairs] = jnp.where(hit, 1.0, 0.0).astype(jnp.bfloat16)

    def wide_copy(c, o, to):
        return pltpu.make_async_remote_copy(
            src_ref=sums.at[o, c],
            dst_ref=sums_r.at[o, c],
            send_sem=wide_ss.at[c, o],
            recv_sem=wide_rs.at[c, o],
            device_id={"wide": to},
            device_id_type=MESH,
        )

    def add_up(c):
        pieces = [terms_r[:, c, j].reshape(narrow * pairs, lanes) for j in range(part)]
        received = jnp.concatenate(pieces, axis=1)
        for o in [0, 4, 1, 3, 2]:
            total = jnp.dot(select[o], received, preferred_element_type=jnp.float32)
            for j in range(part):
                piece = total[:, j * lanes : (j + 1) * lanes]
                if o == REACH:
                    own[c, j] = piece
                else:
                    sums[o, c, j] = piece.astype(jnp.bfloat16)
            if o != REACH:
                wide_copy(c, o, on_wide(o - REACH)).start()

    for b in range(batches):
        own_copy(b).wait()
        for step in range(1, narrow):
            peer = on_narrow(step)
            term_copy(b, 0, peer, peer).wait_recv()
    for c in range(comps - 1):
        add_up(c)
    own_late.wait()
    for step in range(1, narrow):
        peer = on_narrow(step)
        late_copy(0, peer, peer).wait_recv()
    add_up(comps - 1)

    def total_of(c):
        total = own[c]
        for o in shifts:
            wide_copy(c, o, on_wide(REACH - o)).wait_recv()
            total = total + sums_r[o, c].astype(jnp.float32)
        return total

    wet_total = total_of(0)
    covered = wet_total > WET_LIMIT
    safe = jnp.where(covered, wet_total, 1.0)
    for v in range(variables):
        result = jnp.where(covered, total_of(v + 1) / safe, 0.0)
        out_ref[v] = result.astype(out_ref.dtype)

    for copy in field_out + target_out:
        copy.wait_send()
    for step in order:
        for b in range(batches):
            term_copy(b, step, on_narrow(step), n).wait_send()
        late_copy(step, on_narrow(step), n).wait_send()
    for c in range(comps):
        for o in shifts:
            wide_copy(c, o, on_wide(o - REACH)).wait_send()


def per_device(wide, narrow, src_field, src_depth, packed_counts, pair_source, pair_home, pair_count):
    variables, part, _ = src_field.shape
    pairs, _, lanes = packed_counts.shape
    own_tiles = src_depth.shape[0] // lanes
    levels = narrow * part
    comps = variables + 1
    offsets = 2 * REACH + 1
    batches = pairs // BATCH
    dma = pltpu.SemaphoreType.DMA
    bf16, f32, i32 = jnp.bfloat16, jnp.float32, jnp.int32
    anywhere = pl.BlockSpec(memory_space=pl.ANY)
    result = pl.pallas_call(
        functools.partial(kernel, wide, narrow),
        out_shape=jax.ShapeDtypeStruct((variables, part, TB_DEV, lanes), bf16),
        in_specs=[anywhere] * 6,
        out_specs=pl.BlockSpec(memory_space=pltpu.VMEM),
        scratch_shapes=[
            pltpu.VMEM(src_field.shape, bf16),
            pltpu.VMEM((own_tiles, lanes), i32),
            pltpu.VMEM(packed_counts.shape, i32),
            pltpu.VMEM((1, pairs), i32),
            pltpu.SMEM((pairs,), i32),
            pltpu.SMEM((1,), i32),
            pltpu.VMEM((1, 1, pairs), i32),
            pltpu.VMEM((narrow, 1, pairs), i32),
            pltpu.VMEM((narrow, variables, part, own_tiles * lanes), bf16),
            pltpu.VMEM((own_tiles, variables * levels, lanes), f32),
            pltpu.VMEM((own_tiles, comps * levels, lanes), bf16),
            pltpu.VMEM((comps * levels * PITCH, lanes), f32),
            pltpu.VMEM((narrow, comps, part, pairs, lanes), bf16),
            pltpu.VMEM((narrow, comps, part, pairs, lanes), bf16),
            pltpu.VMEM((offsets, TB_DEV, narrow * pairs), bf16),
            pltpu.VMEM((offsets, comps, part, TB_DEV, lanes), bf16),
            pltpu.VMEM((comps, part, TB_DEV, lanes), f32),
            pltpu.VMEM((offsets, comps, part, TB_DEV, lanes), bf16),
            dma((5,)),
            dma((batches,)),
            dma(()),
            dma((narrow,)),
            dma((narrow,)),
            dma((narrow,)),
            dma((narrow,)),
            dma((batches, narrow)),
            dma((batches, narrow)),
            dma((batches,)),
            dma((narrow,)),
            dma((narrow,)),
            dma(()),
            dma((comps, offsets)),
            dma((comps, offsets)),
        ],
        compiler_params=pltpu.CompilerParams(collective_id=0, has_side_effects=True),
    )(
        src_field,
        src_depth.reshape(own_tiles, lanes),
        packed_counts,
        pair_source,
        pair_home.reshape(1, pairs),
        pair_count,
    )
    return result.reshape(variables, part, TB_DEV * lanes)


def solution(mesh):
    both = ("wide", "narrow")
    return jax.shard_map(
        functools.partial(per_device, mesh.shape["wide"], mesh.shape["narrow"]),
        mesh=mesh,
        in_specs=(P(None, "narrow", "wide"), P(both), P(both, None, None), P(both), P(both), P(both)),
        out_specs=P(None, "narrow", "wide"),
        check_vma=False,
    )
```

```python
import functools

import jax
import jax.numpy as jnp
from jax import lax
from jax.experimental import pallas as pl
from jax.experimental.pallas import tpu as pltpu
from jax.sharding import PartitionSpec as P

DENOM = 256
REACH = 2
TB_DEV = 64
WET_LIMIT = 0.001
BATCH = 32
PITCH = 40
MESH = pl.DeviceIdType.MESH


def kernel(
    wide,
    narrow,
    field_in,
    depth_in,
    counts_in,
    source_in,
    home_in,
    live_in,
    out_ref,
    field_v,
    depth_v,
    counts_v,
    home_v,
    source_s,
    live_s,
    target_v,
    target_r,
    field_r,
    rows_f,
    wet_tiles,
    field_tiles,
    wet_spread,
    field_spread,
    paired,
    terms,
    terms_r,
    select,
    sums,
    own,
    sums_r,
    local_sem,
    counts_sem,
    self_sem,
    field_ss,
    field_rs,
    target_ss,
    target_rs,
    wet_ss,
    wet_rs,
    wet_own,
    early_ss,
    early_rs,
    early_own,
    late_ss,
    late_rs,
    late_own,
    wide_ss,
    wide_rs,
):
    w = lax.axis_index("wide")
    n = lax.axis_index("narrow")
    pairs, half, lanes = counts_v.shape
    batches = pairs // BATCH
    own_tiles = wet_tiles.shape[0]
    own_cells = own_tiles * lanes
    variables, part = field_v.shape[0], field_v.shape[1]
    levels = narrow * part
    comps = variables + 1
    offsets = 2 * REACH + 1
    shifts = [o for o in range(offsets) if o != REACH]

    def on_narrow(step):
        return lax.rem(n + step, narrow)

    def on_wide(shift):
        return lax.rem(w + shift + wide, wide)

    first = [
        pltpu.make_async_copy(field_in, field_v, local_sem.at[0]),
        pltpu.make_async_copy(home_in, home_v, local_sem.at[1]),
        pltpu.make_async_copy(live_in, live_s, local_sem.at[2]),
        pltpu.make_async_copy(depth_in, depth_v, local_sem.at[3]),
        pltpu.make_async_copy(source_in, source_s, local_sem.at[4]),
    ]
    for copy in first:
        copy.start()

    def counts_copy(b):
        rows = pl.ds(b * BATCH, BATCH)
        return pltpu.make_async_copy(counts_in.at[rows], counts_v.at[rows], counts_sem.at[b])

    for b in range(batches):
        counts_copy(b).start()

    barrier = pltpu.get_barrier_semaphore()
    for step in range(1, narrow):
        pl.semaphore_signal(barrier, inc=1, device_id={"narrow": on_narrow(step)}, device_id_type=MESH)
    for o in shifts:
        pl.semaphore_signal(barrier, inc=1, device_id={"wide": on_wide(o - REACH)}, device_id_type=MESH)

    first[1].wait()
    first[2].wait()
    home = home_v[...]
    slot = lax.broadcasted_iota(jnp.int32, home.shape, 1)
    offset = lax.rem(home // TB_DEV - w + REACH + wide, wide)
    target = jnp.where(slot < live_s[0, 0], offset * TB_DEV + lax.rem(home, TB_DEV), -1)
    target_v[0] = target
    target_r[n] = target
    first[0].wait()
    pl.semaphore_wait(barrier, narrow - 1 + len(shifts))

    order = [2, 6, 4, 3, 7, 5, 1]
    field_out = []
    target_out = []
    for step in order:
        peer = on_narrow(step)
        cells = pl.ds(pl.multiple_of(peer * own_cells, own_cells), own_cells)
        field_out.append(
            pltpu.make_async_remote_copy(
                src_ref=field_v.at[:, :, cells],
                dst_ref=field_r.at[n],
                send_sem=field_ss.at[step],
                recv_sem=field_rs.at[n],
                device_id={"narrow": peer},
                device_id_type=MESH,
            )
        )
        field_out[-1].start()
    for step in order:
        target_out.append(
            pltpu.make_async_remote_copy(
                src_ref=target_v,
                dst_ref=target_r.at[pl.ds(n, 1)],
                send_sem=target_ss.at[step],
                recv_sem=target_rs.at[n],
                device_id={"narrow": on_narrow(step)},
                device_id_type=MESH,
            )
        )
        target_out[-1].start()
    own_span = pl.ds(pl.multiple_of(n * own_cells, own_cells), own_cells)
    own_field = pltpu.make_async_copy(field_v.at[:, :, own_span], field_r.at[n], self_sem)
    own_field.start()

    def field_from(peer):
        return pltpu.make_async_remote_copy(
            src_ref=field_r.at[peer],
            dst_ref=field_r.at[peer],
            send_sem=field_ss.at[0],
            recv_sem=field_rs.at[peer],
            device_id={"narrow": peer},
            device_id_type=MESH,
        )


    def terms_of(b, stored, spread):
        comps_rows = stored.shape[1]

        def one_pair(i, carry):
            p = b * BATCH + i
            words = counts_v[p]
            low = (words & 65535).astype(jnp.float32) * (1.0 / DENOM)
            high = lax.shift_right_logical(words, 16).astype(jnp.float32) * (1.0 / DENOM)
            weight = jnp.concatenate([low.astype(jnp.bfloat16), high.astype(jnp.bfloat16)], axis=0)
            term = lax.dot_general(
                stored[source_s[p]], weight, (((1,), (1,)), ((), ())), preferred_element_type=jnp.float32
            )
            spread[pl.ds(i, comps_rows, stride=PITCH), :] = term
            return carry

        lax.fori_loop(0, BATCH, one_pair, 0, unroll=8)

    def store_terms(b, c, r0, spread):
        rows = pl.ds(pl.multiple_of(b * BATCH, BATCH), BATCH)
        for l in range(levels):
            r = r0 + l
            block = spread[r * PITCH : r * PITCH + BATCH, :].astype(jnp.bfloat16)
            terms[l // part, c, l % part, rows, :] = block

    def term_copy(c, b, step, peer, to):
        rows = pl.ds(pl.multiple_of(b * BATCH, BATCH), BATCH)
        return pltpu.make_async_remote_copy(
            src_ref=terms.at[peer, c, :, rows],
            dst_ref=terms_r.at[to, c, :, rows],
            send_sem=(wet_ss, early_ss)[c].at[b, step],
            recv_sem=(wet_rs, early_rs)[c].at[b, to],
            device_id={"narrow": peer},
            device_id_type=MESH,
        )

    def own_copy(c, b):
        rows = pl.ds(pl.multiple_of(b * BATCH, BATCH), BATCH)
        return pltpu.make_async_copy(
            terms.at[n, c, :, rows], terms_r.at[n, c, :, rows], (wet_own, early_own)[c].at[b]
        )

    first[3].wait()
    first[4].wait()
    level_ids = lax.broadcasted_iota(jnp.int32, (levels, lanes), 0)
    for s in range(own_tiles):
        wet = level_ids < depth_v[s : s + 1, :]
        wet_tiles[s] = jnp.where(wet, 1.0, 0.0).astype(jnp.bfloat16)

    def wet_batch(b, carry):
        counts_copy(b).wait()
        terms_of(b, wet_tiles, wet_spread)
        store_terms(b, 0, 0, wet_spread)
        for step in order:
            term_copy(0, b, step, on_narrow(step), n).start()
        own_copy(0, b).start()
        return carry

    lax.fori_loop(0, batches, wet_batch, 0)

    own_field.wait()
    for step in range(1, narrow):
        field_from(on_narrow(step)).wait_recv()
    for m in range(narrow):
        for v in range(variables):
            for s in range(own_tiles):
                piece = field_r[m, v, :, s * lanes : (s + 1) * lanes]
                rows_f[s, v * levels + m * part : v * levels + (m + 1) * part, :] = piece.astype(jnp.float32)
    for s in range(own_tiles):
        wet = level_ids < depth_v[s : s + 1, :]
        for v in range(variables):
            rows = rows_f[s, v * levels : (v + 1) * levels, :]
            field_tiles[s, v * levels : (v + 1) * levels, :] = jnp.where(wet, rows, 0.0).astype(jnp.bfloat16)

    def field_batch(b, carry):
        terms_of(b, field_tiles, field_spread)
        for v in range(variables):
            store_terms(b, v + 1, v * levels, field_spread)
        for step in order:
            term_copy(1, b, step, on_narrow(step), n).start()
        own_copy(1, b).start()
        return carry

    lax.fori_loop(0, batches, field_batch, 0)

    def late_copy(j, step, peer, to):
        return pltpu.make_async_remote_copy(
            src_ref=terms.at[peer, comps - 1, j],
            dst_ref=terms_r.at[to, comps - 1, j],
            send_sem=late_ss.at[j, step],
            recv_sem=late_rs.at[j, to],
            device_id={"narrow": peer},
            device_id_type=MESH,
        )

    own_late = pltpu.make_async_copy(terms.at[n, comps - 1], terms_r.at[n, comps - 1], late_own)
    own_late.start()
    for j in range(part):
        for step in order:
            late_copy(j, step, on_narrow(step), n).start()

    for step in range(1, narrow):
        peer = on_narrow(step)
        pltpu.make_async_remote_copy(
            src_ref=target_v,
            dst_ref=target_r.at[pl.ds(peer, 1)],
            send_sem=target_ss.at[0],
            recv_sem=target_rs.at[peer],
            device_id={"narrow": peer},
            device_id_type=MESH,
        ).wait_recv()
    for m in range(narrow):
        for o in range(offsets):
            ids = o * TB_DEV + lax.broadcasted_iota(jnp.int32, (TB_DEV, pairs), 0)
            hit = ids == target_r[m]
            select[o, :, m * pairs : (m + 1) * pairs] = jnp.where(hit, 1.0, 0.0).astype(jnp.bfloat16)

    def wide_copy(u, o, to):
        c, rows = chunks[u]
        return pltpu.make_async_remote_copy(
            src_ref=sums.at[o, c, rows],
            dst_ref=sums_r.at[o, c, rows],
            send_sem=wide_ss.at[u, o],
            recv_sem=wide_rs.at[u, o],
            device_id={"wide": to},
            device_id_type=MESH,
        )

    chunks = [(c, pl.ds(0, part)) for c in range(comps - 1)] + [(comps - 1, pl.ds(j, 1)) for j in range(part)]

    def add_up(u):
        c, rows = chunks[u]
        pieces = [terms_r[:, c, j].reshape(narrow * pairs, lanes) for j in range(rows.start, rows.start + rows.size)]
        received = jnp.concatenate(pieces, axis=1) if len(pieces) > 1 else pieces[0]
        for o in [4, 0, 3, 1, 2]:
            total = jnp.dot(select[o], received, preferred_element_type=jnp.float32)
            for k in range(rows.size):
                piece = total[:, k * lanes : (k + 1) * lanes]
                if o == REACH:
                    own[c, rows.start + k] = piece
                else:
                    sums[o, c, rows.start + k] = piece.astype(jnp.bfloat16)
            if o != REACH:
                wide_copy(u, o, on_wide(o - REACH)).start()

    for c in range(comps - 1):
        for b in range(batches):
            own_copy(c, b).wait()
            for step in range(1, narrow):
                peer = on_narrow(step)
                term_copy(c, b, 0, peer, peer).wait_recv()
        add_up(c)
    own_late.wait()
    for j in range(part):
        for step in range(1, narrow):
            peer = on_narrow(step)
            late_copy(j, 0, peer, peer).wait_recv()
        add_up(comps - 1 + j)

    def total_of(u):
        c, rows = chunks[u]
        total = own[c, rows]
        for o in shifts:
            wide_copy(u, o, on_wide(REACH - o)).wait_recv()
            total = total + sums_r[o, c, rows].astype(jnp.float32)
        return total

    def put(v, j, result):
        paired[v, pl.ds(j, TB_DEV, stride=part), :] = result

    wet_total = total_of(0)
    covered = wet_total > WET_LIMIT
    safe = jnp.where(covered, wet_total, 1.0)
    result = jnp.where(covered, total_of(1) / safe, 0.0)
    for j in range(part):
        put(0, j, result[j])
    for j in range(part):
        put(1, j, jnp.where(covered[j], total_of(comps - 1 + j)[0] / safe[j], 0.0))
    for v in range(variables):
        for t in range(TB_DEV):
            out_ref[v, :, t * lanes : (t + 1) * lanes] = paired[v, t * part : (t + 1) * part, :].astype(out_ref.dtype)

    for copy in field_out + target_out:
        copy.wait_send()
    for step in order:
        for c in range(comps - 1):
            for b in range(batches):
                term_copy(c, b, step, on_narrow(step), n).wait_send()
        for j in range(part):
            late_copy(j, step, on_narrow(step), n).wait_send()
    for u in range(len(chunks)):
        for o in shifts:
            wide_copy(u, o, on_wide(o - REACH)).wait_send()


def per_device(wide, narrow, src_field, src_depth, packed_counts, pair_source, pair_home, pair_count):
    variables, part, _ = src_field.shape
    pairs, _, lanes = packed_counts.shape
    own_tiles = src_depth.shape[0] // lanes
    levels = narrow * part
    comps = variables + 1
    offsets = 2 * REACH + 1
    batches = pairs // BATCH
    dma = pltpu.SemaphoreType.DMA
    bf16, f32, i32 = jnp.bfloat16, jnp.float32, jnp.int32
    in_hbm = pl.BlockSpec(memory_space=pltpu.HBM)
    return pl.pallas_call(
        functools.partial(kernel, wide, narrow),
        out_shape=jax.ShapeDtypeStruct((variables, part, TB_DEV * lanes), bf16),
        in_specs=[in_hbm] * 6,
        out_specs=pl.BlockSpec(memory_space=pltpu.VMEM),
        scratch_shapes=[
            pltpu.VMEM(src_field.shape, bf16),
            pltpu.VMEM((own_tiles, lanes), i32),
            pltpu.VMEM(packed_counts.shape, i32),
            pltpu.VMEM((1, pairs), i32),
            pltpu.SMEM((pairs,), i32),
            pltpu.SMEM((1, 1), i32),
            pltpu.VMEM((1, 1, pairs), i32),
            pltpu.VMEM((narrow, 1, pairs), i32),
            pltpu.VMEM((narrow, variables, part, own_tiles * lanes), bf16),
            pltpu.VMEM((own_tiles, variables * levels, lanes), f32),
            pltpu.VMEM((own_tiles, levels, lanes), bf16),
            pltpu.VMEM((own_tiles, variables * levels, lanes), bf16),
            pltpu.VMEM((levels * PITCH, lanes), f32),
            pltpu.VMEM((variables * levels * PITCH, lanes), f32),
            pltpu.VMEM((variables, TB_DEV * part, lanes), f32),
            pltpu.VMEM((narrow, comps, part, pairs, lanes), bf16),
            pltpu.VMEM((narrow, comps, part, pairs, lanes), bf16),
            pltpu.VMEM((offsets, TB_DEV, narrow * pairs), bf16),
            pltpu.VMEM((offsets, comps, part, TB_DEV, lanes), bf16),
            pltpu.VMEM((comps, part, TB_DEV, lanes), f32),
            pltpu.VMEM((offsets, comps, part, TB_DEV, lanes), bf16),
            dma((5,)),
            dma((batches,)),
            dma(()),
            dma((narrow,)),
            dma((narrow,)),
            dma((narrow,)),
            dma((narrow,)),
            dma((batches, narrow)),
            dma((batches, narrow)),
            dma((batches,)),
            dma((batches, narrow)),
            dma((batches, narrow)),
            dma((batches,)),
            dma((part, narrow)),
            dma((part, narrow)),
            dma(()),
            dma((comps - 1 + part, offsets)),
            dma((comps - 1 + part, offsets)),
        ],
        compiler_params=pltpu.CompilerParams(collective_id=0, has_side_effects=True),
    )(
        src_field,
        src_depth.reshape(own_tiles, lanes),
        packed_counts,
        pair_source,
        pair_home.reshape(1, pairs),
        pair_count.reshape(1, 1),
    )


def solution(mesh):
    both = ("wide", "narrow")
    return jax.shard_map(
        functools.partial(per_device, mesh.shape["wide"], mesh.shape["narrow"]),
        mesh=mesh,
        in_specs=(P(None, "narrow", "wide"), P(both), P(both, None, None), P(both), P(both), P(both)),
        out_specs=P(None, "narrow", "wide"),
        check_vma=False,
    )
```

```python
import functools

import jax
import jax.numpy as jnp
from jax import lax
from jax.experimental import pallas as pl
from jax.experimental.pallas import tpu as pltpu
from jax.sharding import PartitionSpec as P

DENOM = 256
REACH = 2
TB_DEV = 64
WET_LIMIT = 0.001
CAP = 51
BATCH = 32
PITCH = 56
SEGMENTS = ((0, 64), (64, 48), (112, 16))
PIECES = ((0, 32), (32, 32), (64, 48), (112, 16))
MESH = pl.DeviceIdType.MESH


def kernel(
    wide,
    narrow,
    field_in,
    depth_in,
    counts_in,
    source_in,
    home_in,
    live_in,
    out_ref,
    field_v,
    depth_v,
    counts_v,
    home_v,
    source_s,
    live_s,
    order_v,
    order_s,
    target_v,
    target_r,
    field_r,
    rows_f,
    wet_tiles,
    field_tiles,
    wet_spread,
    field_spread,
    paired,
    terms,
    terms_r,
    select_0,
    select_1,
    select_2,
    sums,
    partial,
    sums_r,
    local_sem,
    counts_sem,
    order_sem,
    self_sem,
    field_ss,
    field_rs,
    target_ss,
    target_rs,
    wet_ss,
    wet_rs,
    wet_own,
    var_ss,
    var_rs,
    var_own,
    last_ss,
    last_rs,
    last_own,
    wide_ss,
    wide_rs,
):
    w = lax.axis_index("wide")
    n = lax.axis_index("narrow")
    pairs, half, lanes = counts_v.shape
    batches = pairs // BATCH
    column = lax.rem(w, 8)
    own_tiles = wet_tiles.shape[0]
    own_cells = own_tiles * lanes
    variables, part = field_v.shape[0], field_v.shape[1]
    levels = narrow * part
    comps = variables + 1
    offsets = 2 * REACH + 1
    shifts = [o for o in range(offsets) if o != REACH]
    middle = (column // 4) * (1 - lax.rem(column // 2, 2))
    edge = (column // 4) * lax.rem(column // 2, 2) * lax.rem(column, 2)
    first_off = 4 - 4 * middle - edge
    second_off = 3 - 2 * middle + edge
    third_off = 4 * middle
    fourth_off = 1 + 2 * middle

    def on_narrow(step):
        return lax.rem(n + step, narrow)

    def on_wide(shift):
        return lax.rem(w + shift + wide, wide)

    first = [
        pltpu.make_async_copy(field_in, field_v, local_sem.at[0]),
        pltpu.make_async_copy(home_in, home_v, local_sem.at[1]),
        pltpu.make_async_copy(live_in, live_s, local_sem.at[2]),
        pltpu.make_async_copy(depth_in, depth_v, local_sem.at[3]),
        pltpu.make_async_copy(source_in, source_s, local_sem.at[4]),
    ]
    for copy in first:
        copy.start()

    def counts_copy(b):
        rows = pl.ds(b * BATCH, BATCH)
        return pltpu.make_async_copy(counts_in.at[rows], counts_v.at[rows], counts_sem.at[b])

    for b in range(batches):
        counts_copy(b).start()

    barrier = pltpu.get_barrier_semaphore()
    for step in range(1, narrow):
        pl.semaphore_signal(barrier, inc=1, device_id={"narrow": on_narrow(step)}, device_id_type=MESH)
    for o in shifts:
        pl.semaphore_signal(barrier, inc=1, device_id={"wide": on_wide(o - REACH)}, device_id_type=MESH)

    first[1].wait()
    first[2].wait()
    home = home_v[...]
    slot = lax.broadcasted_iota(jnp.int32, home.shape, 1)
    offset = lax.rem(home // TB_DEV - w + REACH + wide, wide)
    live = slot < live_s[0, 0]
    target = jnp.where(live, offset * TB_DEV + lax.rem(home, TB_DEV), -1)
    turn = jnp.where(offset == first_off, 0, jnp.where(offset == second_off, 1, 2))
    key = jnp.where(live, turn, 3)
    square = (pairs, pairs)
    down = lax.broadcasted_iota(jnp.int32, square, 0)
    across = lax.broadcasted_iota(jnp.int32, square, 1)
    both = key * 1024 + target + 1
    both_across = jnp.broadcast_to(both, square)
    both_down = jnp.transpose(both_across)
    key_across = both_across // 1024
    key_down = both_down // 1024
    ahead = (key_down < key_across) | ((key_down == key_across) & (down < across))
    rank = jnp.sum(jnp.where(ahead, 1, 0), axis=0, keepdims=True)
    rank_down = jnp.transpose(jnp.broadcast_to(rank, square))
    chosen = rank_down == across
    order_v[...] = jnp.sum(jnp.where(chosen, down, 0), axis=0, keepdims=True)
    sorted_target = jnp.sum(jnp.where(chosen, lax.rem(both_down, 1024) - 1, 0), axis=0, keepdims=True)
    target_v[0] = sorted_target
    target_r[n] = sorted_target
    first[0].wait()
    pl.semaphore_wait(barrier, narrow - 1 + len(shifts))

    order = [2, 6, 4, 3, 7, 5, 1]
    field_out = []
    target_out = []
    for step in order:
        peer = on_narrow(step)
        cells = pl.ds(pl.multiple_of(peer * own_cells, own_cells), own_cells)
        field_out.append(
            pltpu.make_async_remote_copy(
                src_ref=field_v.at[:, :, cells],
                dst_ref=field_r.at[n],
                send_sem=field_ss.at[step],
                recv_sem=field_rs.at[n],
                device_id={"narrow": peer},
                device_id_type=MESH,
            )
        )
        field_out[-1].start()
    for step in order:
        target_out.append(
            pltpu.make_async_remote_copy(
                src_ref=target_v,
                dst_ref=target_r.at[pl.ds(n, 1)],
                send_sem=target_ss.at[step],
                recv_sem=target_rs.at[n],
                device_id={"narrow": on_narrow(step)},
                device_id_type=MESH,
            )
        )
        target_out[-1].start()
    own_span = pl.ds(pl.multiple_of(n * own_cells, own_cells), own_cells)
    own_field = pltpu.make_async_copy(field_v.at[:, :, own_span], field_r.at[n], self_sem)
    own_field.start()

    def field_from(peer):
        return pltpu.make_async_remote_copy(
            src_ref=field_r.at[peer],
            dst_ref=field_r.at[peer],
            send_sem=field_ss.at[0],
            recv_sem=field_rs.at[peer],
            device_id={"narrow": peer},
            device_id_type=MESH,
        )


    def terms_of(lo, size, stored, spread):
        comps_rows = stored.shape[1]

        def one_pair(i, carry):
            p = order_s[0, lo + i]
            words = counts_v[p]
            low = (words & 65535).astype(jnp.float32) * (1.0 / DENOM)
            high = lax.shift_right_logical(words, 16).astype(jnp.float32) * (1.0 / DENOM)
            weight = jnp.concatenate([low.astype(jnp.bfloat16), high.astype(jnp.bfloat16)], axis=0)
            term = lax.dot_general(
                stored[source_s[p]], weight, (((1,), (1,)), ((), ())), preferred_element_type=jnp.float32
            )
            spread[pl.ds(i, comps_rows, stride=PITCH), :] = term
            return carry

        lax.fori_loop(0, size, one_pair, 0, unroll=8)

    def store_terms(lo, size, c, r0, spread):
        for l in range(levels):
            r = r0 + l
            block = spread[r * PITCH : r * PITCH + size, :].astype(jnp.bfloat16)
            terms[l // part, c, l % part, lo : lo + size, :] = block

    def spans(k):
        lo, size = PIECES[k]
        return lo, lo + size

    def wet_copy(k, step, peer, to):
        lo, hi = spans(k)
        return pltpu.make_async_remote_copy(
            src_ref=terms.at[peer, 0, :, lo:hi],
            dst_ref=terms_r.at[to, 0, :, lo:hi],
            send_sem=wet_ss.at[k, step],
            recv_sem=wet_rs.at[k, to],
            device_id={"narrow": peer},
            device_id_type=MESH,
        )

    def var_copy(k, step, peer, to):
        lo, hi = spans(k)
        return pltpu.make_async_remote_copy(
            src_ref=terms.at[peer, 1:, :, lo:hi],
            dst_ref=terms_r.at[to, 1:, :, lo:hi],
            send_sem=var_ss.at[k, step],
            recv_sem=var_rs.at[k, to],
            device_id={"narrow": peer},
            device_id_type=MESH,
        )

    def last_copy(step, peer, to):
        lo, hi = spans(len(PIECES) - 1)
        return pltpu.make_async_remote_copy(
            src_ref=terms.at[peer, :, :, lo:hi],
            dst_ref=terms_r.at[to, :, :, lo:hi],
            send_sem=last_ss.at[step],
            recv_sem=last_rs.at[to],
            device_id={"narrow": peer},
            device_id_type=MESH,
        )

    def own_copy(k, comp, sem):
        lo, hi = spans(k)
        return pltpu.make_async_copy(terms.at[n, comp, :, lo:hi], terms_r.at[n, comp, :, lo:hi], sem)

    wet_part, var_part, all_parts = slice(0, 1), slice(1, comps), slice(0, comps)
    early = range(len(PIECES) - 1)

    to_scalars = pltpu.make_async_copy(order_v, order_s, order_sem)
    to_scalars.start()
    first[3].wait()
    first[4].wait()
    level_ids = lax.broadcasted_iota(jnp.int32, (levels, lanes), 0)
    for s in range(own_tiles):
        wet = level_ids < depth_v[s : s + 1, :]
        wet_tiles[s] = jnp.where(wet, 1.0, 0.0).astype(jnp.bfloat16)
    for b in range(batches):
        counts_copy(b).wait()
    to_scalars.wait()

    for k in early:
        terms_of(*PIECES[k], wet_tiles, wet_spread)
        store_terms(*PIECES[k], 0, 0, wet_spread)
        for step in order:
            wet_copy(k, step, on_narrow(step), n).start()
        own_copy(k, wet_part, wet_own.at[k]).start()
    terms_of(*PIECES[-1], wet_tiles, wet_spread)
    store_terms(*PIECES[-1], 0, 0, wet_spread)

    own_field.wait()
    for step in range(1, narrow):
        field_from(on_narrow(step)).wait_recv()
    for m in range(narrow):
        for v in range(variables):
            for s in range(own_tiles):
                piece = field_r[m, v, :, s * lanes : (s + 1) * lanes]
                rows_f[s, v * levels + m * part : v * levels + (m + 1) * part, :] = piece.astype(jnp.float32)
    for s in range(own_tiles):
        wet = level_ids < depth_v[s : s + 1, :]
        for v in range(variables):
            rows = rows_f[s, v * levels : (v + 1) * levels, :]
            field_tiles[s, v * levels : (v + 1) * levels, :] = jnp.where(wet, rows, 0.0).astype(jnp.bfloat16)

    for k in range(len(PIECES)):
        terms_of(*PIECES[k], field_tiles, field_spread)
        for v in range(variables):
            store_terms(*PIECES[k], v + 1, v * levels, field_spread)
        if k in early:
            for step in order:
                var_copy(k, step, on_narrow(step), n).start()
            own_copy(k, var_part, var_own.at[k]).start()
        else:
            for step in order:
                last_copy(step, on_narrow(step), n).start()
            own_copy(k, all_parts, last_own).start()

    for step in range(1, narrow):
        peer = on_narrow(step)
        pltpu.make_async_remote_copy(
            src_ref=target_v,
            dst_ref=target_r.at[pl.ds(peer, 1)],
            send_sem=target_ss.at[0],
            recv_sem=target_rs.at[peer],
            device_id={"narrow": peer},
            device_id_type=MESH,
        ).wait_recv()
    lane_ids = lax.broadcasted_iota(jnp.int32, (1, lanes), 1)
    selects = (select_0, select_1, select_2)
    for (lo, size), select in zip(SEGMENTS, selects):
        for k in range(narrow * size // lanes):
            row = jnp.full((1, lanes), -1, jnp.int32)
            for m in range(narrow):
                start = m * size - k * lanes
                left, right = max(0, start), min(lanes, start + size)
                if left < right:
                    turned = pltpu.roll(target_r[m], (start - lo) % lanes, 1)
                    row = jnp.where((lane_ids >= left) & (lane_ids < right), turned, row)
            for o in range(offsets):
                ids = o * TB_DEV + lax.broadcasted_iota(jnp.int32, (TB_DEV, lanes), 0)
                hit = jnp.where(ids == row, 1.0, 0.0).astype(jnp.bfloat16)
                select[o, :, k * lanes : (k + 1) * lanes] = hit

    def wide_copy(c, o, to):
        return pltpu.make_async_remote_copy(
            src_ref=sums.at[o, c],
            dst_ref=sums_r.at[o, c],
            send_sem=wide_ss.at[c, o],
            recv_sem=wide_rs.at[c, o],
            device_id={"wide": to},
            device_id_type=MESH,
        )

    def arrived(g, c):
        lo, size = SEGMENTS[g]
        pieces = [terms_r[:, c, j, lo : lo + size].reshape(narrow * size, lanes) for j in range(part)]
        return jnp.concatenate(pieces, axis=1)

    def add_up(g, c, o, received, done):
        total = jnp.dot(selects[g][o], received, preferred_element_type=jnp.float32)
        for j in range(part):
            piece = total[:, j * lanes : (j + 1) * lanes]
            if g > 0:
                piece = partial[o, c, j] + piece
            if done:
                sums[o, c, j] = piece.astype(jnp.bfloat16)
            else:
                partial[o, c, j] = piece
        if done:
            wide_copy(c, o, on_wide(o - REACH)).start()

    def wait_pieces(which):
        for k in which:
            own_copy(k, wet_part, wet_own.at[k]).wait()
            own_copy(k, var_part, var_own.at[k]).wait()
            for step in range(1, narrow):
                peer = on_narrow(step)
                wet_copy(k, 0, peer, peer).wait_recv()
                var_copy(k, 0, peer, peer).wait_recv()

    wait_pieces([0, 1])
    for c in range(comps):
        add_up(0, c, first_off, arrived(0, c), True)
    for c in range(comps):
        for o in (second_off, third_off, fourth_off, REACH):
            add_up(0, c, o, arrived(0, c), False)
    wait_pieces([2])
    for c in range(comps):
        add_up(1, c, second_off, arrived(1, c), True)
    for c in range(comps):
        for o in (third_off, fourth_off, REACH):
            add_up(1, c, o, arrived(1, c), False)
    own_copy(len(PIECES) - 1, all_parts, last_own).wait()
    for step in range(1, narrow):
        peer = on_narrow(step)
        last_copy(0, peer, peer).wait_recv()
    for c in range(comps):
        add_up(2, c, third_off, arrived(2, c), True)
        add_up(2, c, fourth_off, arrived(2, c), True)
    for c in range(comps):
        add_up(2, c, REACH, arrived(2, c), False)

    def total_of(c):
        total = partial[REACH, c]
        for o in shifts:
            wide_copy(c, o, on_wide(REACH - o)).wait_recv()
            total = total + sums_r[o, c].astype(jnp.float32)
        return total

    wet_total = total_of(0)
    covered = wet_total > WET_LIMIT
    safe = jnp.where(covered, wet_total, 1.0)
    for v in range(variables):
        result = jnp.where(covered, total_of(v + 1) / safe, 0.0)
        for j in range(part):
            paired[v, pl.ds(j, TB_DEV, stride=part), :] = result[j]
        for t in range(TB_DEV):
            out_ref[v, :, t * lanes : (t + 1) * lanes] = paired[v, t * part : (t + 1) * part, :].astype(out_ref.dtype)

    for copy in field_out + target_out:
        copy.wait_send()
    for step in order:
        for k in early:
            wet_copy(k, step, on_narrow(step), n).wait_send()
            var_copy(k, step, on_narrow(step), n).wait_send()
        last_copy(step, on_narrow(step), n).wait_send()
    for c in range(comps):
        for o in shifts:
            wide_copy(c, o, on_wide(o - REACH)).wait_send()


def per_device(wide, narrow, src_field, src_depth, packed_counts, pair_source, pair_home, pair_count):
    variables, part, _ = src_field.shape
    pairs, _, lanes = packed_counts.shape
    own_tiles = src_depth.shape[0] // lanes
    levels = narrow * part
    comps = variables + 1
    offsets = 2 * REACH + 1
    batches = pairs // BATCH
    early = len(PIECES) - 1
    dma = pltpu.SemaphoreType.DMA
    bf16, f32, i32 = jnp.bfloat16, jnp.float32, jnp.int32
    in_hbm = pl.BlockSpec(memory_space=pltpu.HBM)
    return pl.pallas_call(
        functools.partial(kernel, wide, narrow),
        out_shape=jax.ShapeDtypeStruct((variables, part, TB_DEV * lanes), bf16),
        in_specs=[in_hbm] * 6,
        out_specs=pl.BlockSpec(memory_space=pltpu.VMEM),
        scratch_shapes=[
            pltpu.VMEM(src_field.shape, bf16),
            pltpu.VMEM((own_tiles, lanes), i32),
            pltpu.VMEM(packed_counts.shape, i32),
            pltpu.VMEM((1, pairs), i32),
            pltpu.SMEM((pairs,), i32),
            pltpu.SMEM((1, 1), i32),
            pltpu.VMEM((1, pairs), i32),
            pltpu.SMEM((1, pairs), i32),
            pltpu.VMEM((1, 1, pairs), i32),
            pltpu.VMEM((narrow, 1, pairs), i32),
            pltpu.VMEM((narrow, variables, part, own_tiles * lanes), bf16),
            pltpu.VMEM((own_tiles, variables * levels, lanes), f32),
            pltpu.VMEM((own_tiles, levels, lanes), bf16),
            pltpu.VMEM((own_tiles, variables * levels, lanes), bf16),
            pltpu.VMEM((levels * PITCH, lanes), f32),
            pltpu.VMEM((variables * levels * PITCH, lanes), f32),
            pltpu.VMEM((variables, TB_DEV * part, lanes), f32),
            pltpu.VMEM((narrow, comps, part, pairs, lanes), bf16),
            pltpu.VMEM((narrow, comps, part, pairs, lanes), bf16),
            *[pltpu.VMEM((offsets, TB_DEV, narrow * size), bf16) for _, size in SEGMENTS],
            pltpu.VMEM((offsets, comps, part, TB_DEV, lanes), bf16),
            pltpu.VMEM((offsets, comps, part, TB_DEV, lanes), f32),
            pltpu.VMEM((offsets, comps, part, TB_DEV, lanes), bf16),
            dma((5,)),
            dma((batches,)),
            dma(()),
            dma(()),
            dma((narrow,)),
            dma((narrow,)),
            dma((narrow,)),
            dma((narrow,)),
            dma((early, narrow)),
            dma((early, narrow)),
            dma((early,)),
            dma((early, narrow)),
            dma((early, narrow)),
            dma((early,)),
            dma((narrow,)),
            dma((narrow,)),
            dma(()),
            dma((comps, offsets)),
            dma((comps, offsets)),
        ],
        compiler_params=pltpu.CompilerParams(collective_id=0, has_side_effects=True),
    )(
        src_field,
        src_depth.reshape(own_tiles, lanes),
        packed_counts,
        pair_source,
        pair_home.reshape(1, pairs),
        pair_count.reshape(1, 1),
    )


def solution(mesh):
    both = ("wide", "narrow")
    return jax.shard_map(
        functools.partial(per_device, mesh.shape["wide"], mesh.shape["narrow"]),
        mesh=mesh,
        in_specs=(P(None, "narrow", "wide"), P(both), P(both, None, None), P(both), P(both), P(both)),
        out_specs=P(None, "narrow", "wide"),
        check_vma=False,
    )
```

```python
import functools

import jax
import jax.numpy as jnp
from jax import lax
from jax.experimental import pallas as pl
from jax.experimental.pallas import tpu as pltpu
from jax.sharding import PartitionSpec as P

DENOM = 256
REACH = 2
TB_DEV = 64
WET_LIMIT = 0.001
CAP = 51
BATCH = 32
PITCH = 56
SEGMENTS = ((0, 64), (64, 48), (112, 16))
PIECES = ((0, 32), (32, 32), (64, 48), (112, 16))
MESH = pl.DeviceIdType.MESH


def kernel(
    wide,
    narrow,
    field_in,
    depth_in,
    counts_in,
    source_in,
    home_in,
    live_in,
    out_ref,
    field_v,
    depth_v,
    counts_v,
    home_v,
    source_s,
    live_s,
    order_v,
    order_s,
    target_v,
    target_r,
    field_r,
    rows_f,
    wet_tiles,
    field_tiles,
    wet_spread,
    field_spread,
    paired,
    terms,
    terms_r,
    select_0,
    select_1,
    select_2,
    sums,
    partial,
    sums_r,
    group_in,
    wide_in,
    local_sem,
    counts_sem,
    order_sem,
    self_sem,
    field_ss,
    field_rs,
    target_ss,
    target_rs,
    wet_ss,
    wet_rs,
    wet_own,
    var_ss,
    var_rs,
    var_own,
    last_ss,
    last_rs,
    last_own,
    wide_ss,
    wide_rs,
):
    w = lax.axis_index("wide")
    n = lax.axis_index("narrow")
    pairs, half, lanes = counts_v.shape
    batches = pairs // BATCH
    column = lax.rem(w, 8)
    own_tiles = wet_tiles.shape[0]
    own_cells = own_tiles * lanes
    variables, part = field_v.shape[0], field_v.shape[1]
    levels = narrow * part
    comps = variables + 1
    offsets = 2 * REACH + 1
    shifts = [o for o in range(offsets) if o != REACH]
    middle = (column // 4) * (1 - lax.rem(column // 2, 2))
    edge = (column // 4) * lax.rem(column // 2, 2) * lax.rem(column, 2)
    first_off = 4 - 4 * middle - edge
    second_off = 3 - 2 * middle + edge
    third_off = 4 * middle
    fourth_off = 1 + 2 * middle

    def on_narrow(step):
        return lax.rem(n + step, narrow)

    def on_wide(shift):
        return lax.rem(w + shift + wide, wide)

    first = [
        pltpu.make_async_copy(field_in, field_v, local_sem.at[0]),
        pltpu.make_async_copy(home_in, home_v, local_sem.at[1]),
        pltpu.make_async_copy(live_in, live_s, local_sem.at[2]),
        pltpu.make_async_copy(depth_in, depth_v, local_sem.at[3]),
        pltpu.make_async_copy(source_in, source_s, local_sem.at[4]),
    ]
    for copy in first:
        copy.start()

    def counts_copy(b):
        rows = pl.ds(b * BATCH, BATCH)
        return pltpu.make_async_copy(counts_in.at[rows], counts_v.at[rows], counts_sem.at[b])

    for b in range(batches):
        counts_copy(b).start()

    barrier = pltpu.get_barrier_semaphore()
    core = lax.rem(n, 2)
    twin = n + 1 - 2 * core
    for step in range(2, narrow, 2):
        pl.semaphore_signal(
            barrier, inc=1, device_id={"narrow": lax.rem(n - core + step, narrow)}, device_id_type=MESH
        )
    for o in shifts:
        pl.semaphore_signal(
            barrier,
            inc=1,
            device_id={"wide": on_wide(o - REACH), "narrow": n - core + 1},
            device_id_type=MESH,
        )

    @pl.when(core == 1)
    def _():
        pl.semaphore_signal(barrier, inc=1, device_id={"narrow": twin}, device_id_type=MESH)

    first[1].wait()
    first[2].wait()
    home = home_v[...]
    slot = lax.broadcasted_iota(jnp.int32, home.shape, 1)
    offset = lax.rem(home // TB_DEV - w + REACH + wide, wide)
    live = slot < live_s[0, 0]
    target = jnp.where(live, offset * TB_DEV + lax.rem(home, TB_DEV), -1)
    turn = jnp.where(offset == first_off, 0, jnp.where(offset == second_off, 1, 2))
    key = jnp.where(live, turn, 3)
    square = (pairs, pairs)
    down = lax.broadcasted_iota(jnp.int32, square, 0)
    across = lax.broadcasted_iota(jnp.int32, square, 1)
    both = key * 1024 + target + 1
    both_across = jnp.broadcast_to(both, square)
    both_down = jnp.transpose(both_across)
    key_across = both_across // 1024
    key_down = both_down // 1024
    ahead = (key_down < key_across) | ((key_down == key_across) & (down < across))
    rank = jnp.sum(jnp.where(ahead, 1, 0), axis=0, keepdims=True)
    rank_down = jnp.transpose(jnp.broadcast_to(rank, square))
    chosen = rank_down == across
    order_v[...] = jnp.sum(jnp.where(chosen, down, 0), axis=0, keepdims=True)
    sorted_target = jnp.sum(jnp.where(chosen, lax.rem(both_down, 1024) - 1, 0), axis=0, keepdims=True)
    target_v[0] = sorted_target
    target_r[n] = sorted_target
    first[0].wait()

    @pl.when(core == 0)
    def _():
        pl.semaphore_wait(barrier, narrow - 1)
        pl.semaphore_signal(group_in, inc=1, device_id={"narrow": twin}, device_id_type=MESH)

    @pl.when(core == 1)
    def _():
        pl.semaphore_wait(group_in, 1)


    order = [2, 6, 4, 3, 7, 5, 1]
    field_out = []
    target_out = []
    for step in order:
        peer = on_narrow(step)
        cells = pl.ds(pl.multiple_of(peer * own_cells, own_cells), own_cells)
        field_out.append(
            pltpu.make_async_remote_copy(
                src_ref=field_v.at[:, :, cells],
                dst_ref=field_r.at[n],
                send_sem=field_ss.at[step],
                recv_sem=field_rs.at[n],
                device_id={"narrow": peer},
                device_id_type=MESH,
            )
        )
        field_out[-1].start()
    for step in order:
        target_out.append(
            pltpu.make_async_remote_copy(
                src_ref=target_v,
                dst_ref=target_r.at[pl.ds(n, 1)],
                send_sem=target_ss.at[step],
                recv_sem=target_rs.at[n],
                device_id={"narrow": on_narrow(step)},
                device_id_type=MESH,
            )
        )
        target_out[-1].start()
    own_span = pl.ds(pl.multiple_of(n * own_cells, own_cells), own_cells)
    own_field = pltpu.make_async_copy(field_v.at[:, :, own_span], field_r.at[n], self_sem)
    own_field.start()

    def field_from(peer):
        return pltpu.make_async_remote_copy(
            src_ref=field_r.at[peer],
            dst_ref=field_r.at[peer],
            send_sem=field_ss.at[0],
            recv_sem=field_rs.at[peer],
            device_id={"narrow": peer},
            device_id_type=MESH,
        )


    def terms_of(lo, size, stored, spread):
        comps_rows = stored.shape[1]

        def one_pair(i, carry):
            p = order_s[0, lo + i]
            words = counts_v[p]
            low = (words & 65535).astype(jnp.float32) * (1.0 / DENOM)
            high = lax.shift_right_logical(words, 16).astype(jnp.float32) * (1.0 / DENOM)
            weight = jnp.concatenate([low.astype(jnp.bfloat16), high.astype(jnp.bfloat16)], axis=0)
            term = lax.dot_general(
                stored[source_s[p]], weight, (((1,), (1,)), ((), ())), preferred_element_type=jnp.float32
            )
            spread[pl.ds(i, comps_rows, stride=PITCH), :] = term
            return carry

        lax.fori_loop(0, size, one_pair, 0, unroll=8)

    def store_terms(lo, size, c, r0, spread):
        for l in range(levels):
            r = r0 + l
            block = spread[r * PITCH : r * PITCH + size, :].astype(jnp.bfloat16)
            terms[l // part, c, l % part, lo : lo + size, :] = block

    def spans(k):
        lo, size = PIECES[k]
        return lo, lo + size

    def wet_copy(k, step, peer, to):
        lo, hi = spans(k)
        return pltpu.make_async_remote_copy(
            src_ref=terms.at[peer, 0, :, lo:hi],
            dst_ref=terms_r.at[to, 0, :, lo:hi],
            send_sem=wet_ss.at[k, step],
            recv_sem=wet_rs.at[k, to],
            device_id={"narrow": peer},
            device_id_type=MESH,
        )

    def var_copy(k, step, peer, to):
        lo, hi = spans(k)
        return pltpu.make_async_remote_copy(
            src_ref=terms.at[peer, 1:, :, lo:hi],
            dst_ref=terms_r.at[to, 1:, :, lo:hi],
            send_sem=var_ss.at[k, step],
            recv_sem=var_rs.at[k, to],
            device_id={"narrow": peer},
            device_id_type=MESH,
        )

    def last_copy(step, peer, to):
        lo, hi = spans(len(PIECES) - 1)
        return pltpu.make_async_remote_copy(
            src_ref=terms.at[peer, :, :, lo:hi],
            dst_ref=terms_r.at[to, :, :, lo:hi],
            send_sem=last_ss.at[step],
            recv_sem=last_rs.at[to],
            device_id={"narrow": peer},
            device_id_type=MESH,
        )

    def own_copy(k, comp, sem):
        lo, hi = spans(k)
        return pltpu.make_async_copy(terms.at[n, comp, :, lo:hi], terms_r.at[n, comp, :, lo:hi], sem)

    wet_part, var_part, all_parts = slice(0, 1), slice(1, comps), slice(0, comps)
    early = range(len(PIECES) - 1)

    to_scalars = pltpu.make_async_copy(order_v, order_s, order_sem)
    to_scalars.start()
    first[3].wait()
    first[4].wait()
    level_ids = lax.broadcasted_iota(jnp.int32, (levels, lanes), 0)
    for s in range(own_tiles):
        wet = level_ids < depth_v[s : s + 1, :]
        wet_tiles[s] = jnp.where(wet, 1.0, 0.0).astype(jnp.bfloat16)
    for b in range(batches):
        counts_copy(b).wait()
    to_scalars.wait()

    for k in early:
        terms_of(*PIECES[k], wet_tiles, wet_spread)
        store_terms(*PIECES[k], 0, 0, wet_spread)
        for step in order:
            wet_copy(k, step, on_narrow(step), n).start()
        own_copy(k, wet_part, wet_own.at[k]).start()
    terms_of(*PIECES[-1], wet_tiles, wet_spread)
    store_terms(*PIECES[-1], 0, 0, wet_spread)

    own_field.wait()
    for step in range(1, narrow):
        field_from(on_narrow(step)).wait_recv()
    for m in range(narrow):
        for v in range(variables):
            for s in range(own_tiles):
                piece = field_r[m, v, :, s * lanes : (s + 1) * lanes]
                rows_f[s, v * levels + m * part : v * levels + (m + 1) * part, :] = piece.astype(jnp.float32)
    for s in range(own_tiles):
        wet = level_ids < depth_v[s : s + 1, :]
        for v in range(variables):
            rows = rows_f[s, v * levels : (v + 1) * levels, :]
            field_tiles[s, v * levels : (v + 1) * levels, :] = jnp.where(wet, rows, 0.0).astype(jnp.bfloat16)

    for k in range(len(PIECES)):
        terms_of(*PIECES[k], field_tiles, field_spread)
        for v in range(variables):
            store_terms(*PIECES[k], v + 1, v * levels, field_spread)
        if k in early:
            for step in order:
                var_copy(k, step, on_narrow(step), n).start()
            own_copy(k, var_part, var_own.at[k]).start()
        else:
            for step in order:
                last_copy(step, on_narrow(step), n).start()
            own_copy(k, all_parts, last_own).start()

    for step in range(1, narrow):
        peer = on_narrow(step)
        pltpu.make_async_remote_copy(
            src_ref=target_v,
            dst_ref=target_r.at[pl.ds(peer, 1)],
            send_sem=target_ss.at[0],
            recv_sem=target_rs.at[peer],
            device_id={"narrow": peer},
            device_id_type=MESH,
        ).wait_recv()
    lane_ids = lax.broadcasted_iota(jnp.int32, (1, lanes), 1)
    selects = (select_0, select_1, select_2)
    for (lo, size), select in zip(SEGMENTS, selects):
        for k in range(narrow * size // lanes):
            row = jnp.full((1, lanes), -1, jnp.int32)
            for m in range(narrow):
                start = m * size - k * lanes
                left, right = max(0, start), min(lanes, start + size)
                if left < right:
                    turned = pltpu.roll(target_r[m], (start - lo) % lanes, 1)
                    row = jnp.where((lane_ids >= left) & (lane_ids < right), turned, row)
            for o in range(offsets):
                ids = o * TB_DEV + lax.broadcasted_iota(jnp.int32, (TB_DEV, lanes), 0)
                hit = jnp.where(ids == row, 1.0, 0.0).astype(jnp.bfloat16)
                select[o, :, k * lanes : (k + 1) * lanes] = hit

    def wide_copy(c, o, to):
        return pltpu.make_async_remote_copy(
            src_ref=sums.at[o, c],
            dst_ref=sums_r.at[o, c],
            send_sem=wide_ss.at[c, o],
            recv_sem=wide_rs.at[c, o],
            device_id={"wide": to},
            device_id_type=MESH,
        )

    def arrived(g, c):
        lo, size = SEGMENTS[g]
        pieces = [terms_r[:, c, j, lo : lo + size].reshape(narrow * size, lanes) for j in range(part)]
        return jnp.concatenate(pieces, axis=1)

    def add_up(g, c, o, received, done):
        total = jnp.dot(selects[g][o], received, preferred_element_type=jnp.float32)
        for j in range(part):
            piece = total[:, j * lanes : (j + 1) * lanes]
            if g > 0:
                piece = partial[o, c, j] + piece
            if done:
                sums[o, c, j] = piece.astype(jnp.bfloat16)
            else:
                partial[o, c, j] = piece
        if done:
            wide_copy(c, o, on_wide(o - REACH)).start()

    def wait_pieces(which):
        for k in which:
            own_copy(k, wet_part, wet_own.at[k]).wait()
            own_copy(k, var_part, var_own.at[k]).wait()
            for step in range(1, narrow):
                peer = on_narrow(step)
                wet_copy(k, 0, peer, peer).wait_recv()
                var_copy(k, 0, peer, peer).wait_recv()

    @pl.when(core == 1)
    def _():
        pl.semaphore_wait(barrier, 2 * len(shifts))
        pl.semaphore_signal(wide_in, inc=1, device_id={"narrow": twin}, device_id_type=MESH)

    @pl.when(core == 0)
    def _():
        pl.semaphore_wait(wide_in, 1)

    wait_pieces([0, 1])
    for c in range(comps):
        add_up(0, c, first_off, arrived(0, c), True)
    for c in range(comps):
        for o in (second_off, third_off, fourth_off, REACH):
            add_up(0, c, o, arrived(0, c), False)
    wait_pieces([2])
    for c in range(comps):
        add_up(1, c, second_off, arrived(1, c), True)
    for c in range(comps):
        for o in (third_off, fourth_off, REACH):
            add_up(1, c, o, arrived(1, c), False)
    own_copy(len(PIECES) - 1, all_parts, last_own).wait()
    for step in range(1, narrow):
        peer = on_narrow(step)
        last_copy(0, peer, peer).wait_recv()
    for c in range(comps):
        add_up(2, c, third_off, arrived(2, c), True)
        add_up(2, c, fourth_off, arrived(2, c), True)
    for c in range(comps):
        add_up(2, c, REACH, arrived(2, c), False)

    def total_of(c):
        total = partial[REACH, c]
        for o in shifts:
            wide_copy(c, o, on_wide(REACH - o)).wait_recv()
            total = total + sums_r[o, c].astype(jnp.float32)
        return total

    wet_total = total_of(0)
    covered = wet_total > WET_LIMIT
    safe = jnp.where(covered, wet_total, 1.0)
    for v in range(variables):
        result = jnp.where(covered, total_of(v + 1) / safe, 0.0)
        for j in range(part):
            paired[v, pl.ds(j, TB_DEV, stride=part), :] = result[j]
        for t in range(TB_DEV):
            out_ref[v, :, t * lanes : (t + 1) * lanes] = paired[v, t * part : (t + 1) * part, :].astype(out_ref.dtype)

    for copy in field_out + target_out:
        copy.wait_send()
    for step in order:
        for k in early:
            wet_copy(k, step, on_narrow(step), n).wait_send()
            var_copy(k, step, on_narrow(step), n).wait_send()
        last_copy(step, on_narrow(step), n).wait_send()
    for c in range(comps):
        for o in shifts:
            wide_copy(c, o, on_wide(o - REACH)).wait_send()


def per_device(wide, narrow, src_field, src_depth, packed_counts, pair_source, pair_home, pair_count):
    variables, part, _ = src_field.shape
    pairs, _, lanes = packed_counts.shape
    own_tiles = src_depth.shape[0] // lanes
    levels = narrow * part
    comps = variables + 1
    offsets = 2 * REACH + 1
    batches = pairs // BATCH
    early = len(PIECES) - 1
    dma = pltpu.SemaphoreType.DMA
    bf16, f32, i32 = jnp.bfloat16, jnp.float32, jnp.int32
    in_hbm = pl.BlockSpec(memory_space=pltpu.HBM)
    return pl.pallas_call(
        functools.partial(kernel, wide, narrow),
        out_shape=jax.ShapeDtypeStruct((variables, part, TB_DEV * lanes), bf16),
        in_specs=[in_hbm] * 6,
        out_specs=pl.BlockSpec(memory_space=pltpu.VMEM),
        scratch_shapes=[
            pltpu.VMEM(src_field.shape, bf16),
            pltpu.VMEM((own_tiles, lanes), i32),
            pltpu.VMEM(packed_counts.shape, i32),
            pltpu.VMEM((1, pairs), i32),
            pltpu.SMEM((pairs,), i32),
            pltpu.SMEM((1, 1), i32),
            pltpu.VMEM((1, pairs), i32),
            pltpu.SMEM((1, pairs), i32),
            pltpu.VMEM((1, 1, pairs), i32),
            pltpu.VMEM((narrow, 1, pairs), i32),
            pltpu.VMEM((narrow, variables, part, own_tiles * lanes), bf16),
            pltpu.VMEM((own_tiles, variables * levels, lanes), f32),
            pltpu.VMEM((own_tiles, levels, lanes), bf16),
            pltpu.VMEM((own_tiles, variables * levels, lanes), bf16),
            pltpu.VMEM((levels * PITCH, lanes), f32),
            pltpu.VMEM((variables * levels * PITCH, lanes), f32),
            pltpu.VMEM((variables, TB_DEV * part, lanes), f32),
            pltpu.VMEM((narrow, comps, part, pairs, lanes), bf16),
            pltpu.VMEM((narrow, comps, part, pairs, lanes), bf16),
            *[pltpu.VMEM((offsets, TB_DEV, narrow * size), bf16) for _, size in SEGMENTS],
            pltpu.VMEM((offsets, comps, part, TB_DEV, lanes), bf16),
            pltpu.VMEM((offsets, comps, part, TB_DEV, lanes), f32),
            pltpu.VMEM((offsets, comps, part, TB_DEV, lanes), bf16),
            pltpu.SemaphoreType.REGULAR,
            pltpu.SemaphoreType.REGULAR,
            dma((5,)),
            dma((batches,)),
            dma(()),
            dma(()),
            dma((narrow,)),
            dma((narrow,)),
            dma((narrow,)),
            dma((narrow,)),
            dma((early, narrow)),
            dma((early, narrow)),
            dma((early,)),
            dma((early, narrow)),
            dma((early, narrow)),
            dma((early,)),
            dma((narrow,)),
            dma((narrow,)),
            dma(()),
            dma((comps, offsets)),
            dma((comps, offsets)),
        ],
        compiler_params=pltpu.CompilerParams(collective_id=0, has_side_effects=True),
    )(
        src_field,
        src_depth.reshape(own_tiles, lanes),
        packed_counts,
        pair_source,
        pair_home.reshape(1, pairs),
        pair_count.reshape(1, 1),
    )


def solution(mesh):
    both = ("wide", "narrow")
    return jax.shard_map(
        functools.partial(per_device, mesh.shape["wide"], mesh.shape["narrow"]),
        mesh=mesh,
        in_specs=(P(None, "narrow", "wide"), P(both), P(both, None, None), P(both), P(both), P(both)),
        out_specs=P(None, "narrow", "wide"),
        check_vma=False,
    )
```

```python
import functools

import jax
import jax.numpy as jnp
from jax import lax
from jax.experimental import pallas as pl
from jax.experimental.pallas import tpu as pltpu
from jax.sharding import PartitionSpec as P

DENOM = 256
REACH = 2
TB_DEV = 64
WET_LIMIT = 0.001
FETCH = 32
PIECES = (((0, 64), (64, 64)), ((0, 32), (32, 32), (64, 64)))
MOST = 3
PITCH = 72
MESH = pl.DeviceIdType.MESH

HOP = (1, -1, -1, 1)
FAR = (2, -2, -1, 1)
NEAR = (1, -1, 0, 0)


def kernel(
    wide,
    narrow,
    field_in,
    depth_in,
    counts_in,
    source_in,
    home_in,
    live_in,
    out_ref,
    field_v,
    depth_v,
    counts_v,
    home_v,
    source_s,
    target_v,
    target_r,
    field_r,
    rows_f,
    wet_tiles,
    field_tiles,
    wet_spread,
    field_spread,
    paired,
    terms,
    raw_r,
    select,
    dense_s,
    dense_r,
    partial,
    sums,
    sums_r,
    group_in,
    wide_in,
    local_sem,
    counts_sem,
    self_sem,
    field_ss,
    field_rs,
    target_ss,
    target_rs,
    raw_ss,
    raw_rs,
    dense_ss,
    dense_rs,
    wide_ss,
    wide_rs,
):
    w = lax.axis_index("wide")
    n = lax.axis_index("narrow")
    pairs, half, lanes = counts_v.shape
    own_tiles = wet_tiles.shape[0]
    own_cells = own_tiles * lanes
    variables, part = field_v.shape[0], field_v.shape[1]
    levels = narrow * part
    comps = variables + 1
    offsets = 2 * REACH + 1
    shifts = [o for o in range(offsets) if o != REACH]
    chips = narrow // 2
    core = lax.rem(n, 2)
    chip = n // 2
    other = 1 - core
    twin = 2 * chip + other

    column = lax.rem(w, 8)
    middle = (column // 4) * (1 - lax.rem(column // 2, 2))
    edge = (column // 4) * lax.rem(column // 2, 2) * lax.rem(column, 2)
    urgent = [4 - 4 * middle - edge, 3 - 2 * middle + edge]
    patient = [4 * middle, 1 + 2 * middle]

    def at(hop, c):
        return lax.rem(chip + hop + chips, chips) * 2 + c

    def on_narrow(step):
        return lax.rem(n + step, narrow)

    def on_wide(shift):
        return lax.rem(w + shift + wide, wide)

    first = [
        pltpu.make_async_copy(field_in, field_v, local_sem.at[0]),
        pltpu.make_async_copy(home_in, home_v, local_sem.at[1]),
        pltpu.make_async_copy(depth_in, depth_v, local_sem.at[2]),
        pltpu.make_async_copy(source_in, source_s, local_sem.at[3]),
    ]
    for copy in first:
        copy.start()

    def counts_copy(b):
        rows = pl.ds(b * FETCH, FETCH)
        return pltpu.make_async_copy(counts_in.at[rows], counts_v.at[rows], counts_sem.at[b])

    for b in range(pairs // FETCH):
        counts_copy(b).start()

    barrier = pltpu.get_barrier_semaphore()
    for hop in range(1, chips):
        pl.semaphore_signal(barrier, inc=1, device_id={"narrow": at(hop, 0)}, device_id_type=MESH)
    for o in shifts:
        pl.semaphore_signal(
            barrier, inc=1, device_id={"wide": on_wide(o - REACH), "narrow": at(0, 1)}, device_id_type=MESH
        )

    @pl.when(core == 1)
    def _():
        pl.semaphore_signal(barrier, inc=1, device_id={"narrow": twin}, device_id_type=MESH)

    first[1].wait()
    home = home_v[...]
    slot = lax.broadcasted_iota(jnp.int32, home.shape, 1)
    offset = lax.rem(home // TB_DEV - w + REACH + wide, wide)
    target = jnp.where(slot < live_in[0], offset * TB_DEV + lax.rem(home, TB_DEV), -1)
    target_v[0] = target
    target_r[n] = target
    first[0].wait()

    @pl.when(core == 0)
    def _():
        pl.semaphore_wait(barrier, narrow - 1)
        pl.semaphore_signal(group_in, inc=1, device_id={"narrow": twin}, device_id_type=MESH)

    @pl.when(core == 1)
    def _():
        pl.semaphore_wait(group_in, 1)

    order = [4, 5, 2, 6, 3, 7, 1]

    def field_copy(step, peer, to):
        cells = pl.ds(pl.multiple_of(peer * own_cells, own_cells), own_cells)
        return pltpu.make_async_remote_copy(
            src_ref=field_v.at[:, :, cells],
            dst_ref=field_r.at[to],
            send_sem=field_ss.at[step],
            recv_sem=field_rs.at[to],
            device_id={"narrow": peer},
            device_id_type=MESH,
        )

    def target_copy(step, peer, to):
        return pltpu.make_async_remote_copy(
            src_ref=target_v,
            dst_ref=target_r.at[pl.ds(to, 1)],
            send_sem=target_ss.at[step],
            recv_sem=target_rs.at[to],
            device_id={"narrow": peer},
            device_id_type=MESH,
        )

    for step in order:
        field_copy(step, on_narrow(step), n).start()
    for step in order:
        target_copy(step, on_narrow(step), n).start()
    own_span = pl.ds(pl.multiple_of(n * own_cells, own_cells), own_cells)
    own_field = pltpu.make_async_copy(field_v.at[:, :, own_span], field_r.at[n], self_sem)
    own_field.start()

    def terms_of(lo, size, stored, spread):
        comps_rows = stored.shape[1]

        def one_pair(i, carry):
            p = lo + i
            words = counts_v[p]
            low = (words & 65535).astype(jnp.float32) * (1.0 / DENOM)
            high = lax.shift_right_logical(words, 16).astype(jnp.float32) * (1.0 / DENOM)
            weight = jnp.concatenate([low.astype(jnp.bfloat16), high.astype(jnp.bfloat16)], axis=0)
            term = lax.dot_general(
                stored[source_s[p]], weight, (((1,), (1,)), ((), ())), preferred_element_type=jnp.float32
            )
            spread[pl.ds(i, comps_rows, stride=PITCH), :] = term
            return carry

        lax.fori_loop(0, size, one_pair, 0, unroll=8)

    def store_terms(lo, size, c, r0, spread):
        for l in range(levels):
            r = r0 + l
            block = spread[r * PITCH : r * PITCH + size, :].astype(jnp.bfloat16)
            terms[l // part, c, l % part, lo : lo + size, :] = block

    spans = (slice(0, 1), slice(1, comps))

    def raw_copy(g, k, role, t):
        lo, size = PIECES[g][k]
        if t < 2:
            peer, data, mine = at(HOP[role], t), at(FAR[role], t), core
        else:
            peer, data, mine = twin, at(NEAR[role], other), 2
        return pltpu.make_async_remote_copy(
            src_ref=terms.at[data, spans[g], role % part, lo : lo + size],
            dst_ref=raw_r.at[role, mine, spans[g], lo : lo + size],
            send_sem=raw_ss.at[g, k, role, t],
            recv_sem=raw_rs.at[g, k, role, mine],
            device_id={"narrow": peer},
            device_id_type=MESH,
        )

    def raw_arrival(g, k, role, t):
        lo, size = PIECES[g][k]
        here = raw_r.at[role, t, spans[g], lo : lo + size]
        return pltpu.make_async_remote_copy(
            src_ref=here,
            dst_ref=here,
            send_sem=raw_ss.at[g, k, role, t],
            recv_sem=raw_rs.at[g, k, role, t],
            device_id={"narrow": at(-HOP[role], t) if t < 2 else twin},
            device_id_type=MESH,
        )

    def send_raw(g, k, roles):
        for t in range(3):
            for role in roles:
                raw_copy(g, k, role, t).start()

    def wait_raw(g, roles):
        for k in range(len(PIECES[g])):
            for role in roles:
                for t in range(3):
                    raw_arrival(g, k, role, t).wait_recv()

    first[2].wait()
    first[3].wait()
    level_ids = lax.broadcasted_iota(jnp.int32, (levels, lanes), 0)
    for s in range(own_tiles):
        wet = level_ids < depth_v[s : s + 1, :]
        wet_tiles[s] = jnp.where(wet, 1.0, 0.0).astype(jnp.bfloat16)
    for k, (lo, size) in enumerate(PIECES[0]):
        for b in range(lo // FETCH, (lo + size) // FETCH):
            counts_copy(b).wait()
        terms_of(lo, size, wet_tiles, wet_spread)
        store_terms(lo, size, 0, 0, wet_spread)
        send_raw(0, k, (0, 1))
        send_raw(0, k, (2, 3))

    own_field.wait()
    for step in range(1, narrow):
        peer = on_narrow(step)
        field_copy(0, peer, peer).wait_recv()
    for m in range(narrow):
        for v in range(variables):
            for s in range(own_tiles):
                piece = field_r[m, v, :, s * lanes : (s + 1) * lanes]
                rows_f[s, v * levels + m * part : v * levels + (m + 1) * part, :] = piece.astype(jnp.float32)
    for s in range(own_tiles):
        wet = level_ids < depth_v[s : s + 1, :]
        for v in range(variables):
            rows = rows_f[s, v * levels : (v + 1) * levels, :]
            field_tiles[s, v * levels : (v + 1) * levels, :] = jnp.where(wet, rows, 0.0).astype(jnp.bfloat16)

    for k, (lo, size) in enumerate(PIECES[1]):
        terms_of(lo, size, field_tiles, field_spread)
        for v in range(variables):
            store_terms(lo, size, v + 1, v * levels, field_spread)
        send_raw(1, k, (0, 1))

    for step in range(1, narrow):
        peer = on_narrow(step)
        target_copy(0, peer, peer).wait_recv()
    for side, hop in enumerate((-1, 1)):
        for q, m in enumerate((at(hop, 0), at(hop, 1), twin, n)):
            row = target_r[m]
            for o in range(offsets):
                ids = o * TB_DEV + lax.broadcasted_iota(jnp.int32, (TB_DEV, pairs), 0)
                hit = jnp.where(ids == row, 1.0, 0.0).astype(jnp.bfloat16)
                select[side, o, :, q * pairs : (q + 1) * pairs] = hit

    def gathered(g, role):
        mine = at(NEAR[role], core)
        columns = []
        for c in range(spans[g].start, spans[g].stop):
            columns.append(
                jnp.concatenate([raw_r[role, t, c] for t in range(3)] + [terms[mine, c, role % part]], axis=0)
            )
        return jnp.concatenate(columns, axis=1) if len(columns) > 1 else columns[0]

    def add_up(role, o, received):
        side = 0 if HOP[role] == 1 else 1
        return jnp.dot(select[side, o], received, preferred_element_type=jnp.float32)

    def dense_copy(g, j, o, peer):
        return pltpu.make_async_remote_copy(
            src_ref=dense_s.at[j, o, spans[g]],
            dst_ref=dense_r.at[j, o, spans[g]],
            send_sem=dense_ss.at[g, j, o],
            recv_sem=dense_rs.at[g, j, o],
            device_id={"narrow": peer},
            device_id_type=MESH,
        )

    def relay(g, o, received):
        for role in (0, 1):
            total = add_up(role, o, received[role])
            for i, c in enumerate(range(spans[g].start, spans[g].stop)):
                dense_s[role, o, c] = total[:, i * lanes : (i + 1) * lanes].astype(jnp.bfloat16)

    def pass_on(g, o):
        for role in (0, 1):
            dense_copy(g, role, o, at(HOP[role], core)).start()

    def gather_own(g, offs):
        received = [gathered(g, role) for role in (2, 3)]
        for o in offs:
            for role in (2, 3):
                total = add_up(role, o, received[role - 2])
                for i, c in enumerate(range(spans[g].start, spans[g].stop)):
                    partial[o, c, role % part] = total[:, i * lanes : (i + 1) * lanes]

    def wide_copy(g, o, to):
        return pltpu.make_async_remote_copy(
            src_ref=sums.at[o, spans[g]],
            dst_ref=sums_r.at[o, spans[g]],
            send_sem=wide_ss.at[g, o],
            recv_sem=wide_rs.at[g, o],
            device_id={"wide": to},
            device_id_type=MESH,
        )

    def finish(g, o, leaves):
        for j in range(part):
            dense_copy(g, j, o, at(-HOP[j], core)).wait_recv()
        for c in range(spans[g].start, spans[g].stop):
            for j in range(part):
                total = partial[o, c, j] + dense_r[j, o, c].astype(jnp.float32)
                if leaves:
                    sums[o, c, j] = total.astype(jnp.bfloat16)
                else:
                    partial[o, c, j] = total
        if leaves:
            wide_copy(g, o, on_wide(o - REACH)).start()

    every = urgent + patient + [REACH]
    wait_raw(0, (0, 1))
    received = [gathered(0, role) for role in (0, 1)]
    for o in urgent:
        relay(0, o, received)
        pass_on(0, o)
    for k in range(len(PIECES[1])):
        send_raw(1, k, (2, 3))
    for o in patient + [REACH]:
        relay(0, o, received)
    wait_raw(0, (2, 3))
    gather_own(0, every)

    wait_raw(1, (0, 1))
    received = [gathered(1, role) for role in (0, 1)]
    for o in urgent:
        relay(1, o, received)
        pass_on(1, o)
    for o in patient + [REACH]:
        pass_on(0, o)
    for o in patient + [REACH]:
        relay(1, o, received)
        pass_on(1, o)

    @pl.when(core == 1)
    def _():
        pl.semaphore_wait(barrier, 2 * len(shifts))
        pl.semaphore_signal(wide_in, inc=1, device_id={"narrow": twin}, device_id_type=MESH)

    @pl.when(core == 0)
    def _():
        pl.semaphore_wait(wide_in, 1)

    for o in urgent:
        finish(0, o, True)
    wait_raw(1, (2, 3))
    gather_own(1, every)
    for o in urgent:
        finish(1, o, True)
    for o in patient:
        finish(0, o, True)
    for o in patient:
        finish(1, o, True)
    for g in range(2):
        finish(g, REACH, False)

    def total_of(c):
        total = partial[REACH, c]
        for o in shifts:
            total = total + sums_r[o, c].astype(jnp.float32)
        return total

    for o in shifts:
        wide_copy(0, o, on_wide(REACH - o)).wait_recv()
    wet_total = total_of(0)
    covered = wet_total > WET_LIMIT
    safe = jnp.where(covered, wet_total, 1.0)
    for o in shifts:
        wide_copy(1, o, on_wide(REACH - o)).wait_recv()
    for v in range(variables):
        result = jnp.where(covered, total_of(v + 1) / safe, 0.0)
        for j in range(part):
            paired[v, pl.ds(j, TB_DEV, stride=part), :] = result[j]
        for t in range(TB_DEV):
            out_ref[v, :, t * lanes : (t + 1) * lanes] = paired[v, t * part : (t + 1) * part, :].astype(out_ref.dtype)

    for step in order:
        field_copy(step, on_narrow(step), n).wait_send()
        target_copy(step, on_narrow(step), n).wait_send()
    for g in range(2):
        for k in range(len(PIECES[g])):
            for role in range(4):
                for t in range(3):
                    raw_copy(g, k, role, t).wait_send()
        for o in range(offsets):
            for role in (0, 1):
                dense_copy(g, role, o, at(HOP[role], core)).wait_send()
        for o in shifts:
            wide_copy(g, o, on_wide(o - REACH)).wait_send()


def per_device(wide, narrow, src_field, src_depth, packed_counts, pair_source, pair_home, pair_count):
    variables, part, _ = src_field.shape
    pairs, _, lanes = packed_counts.shape
    own_tiles = src_depth.shape[0] // lanes
    levels = narrow * part
    comps = variables + 1
    offsets = 2 * REACH + 1
    pieces = MOST
    dma = pltpu.SemaphoreType.DMA
    bf16, f32, i32 = jnp.bfloat16, jnp.float32, jnp.int32
    in_hbm = pl.BlockSpec(memory_space=pltpu.HBM)
    return pl.pallas_call(
        functools.partial(kernel, wide, narrow),
        out_shape=pltpu.VMEM((variables, part, TB_DEV * lanes), bf16),
        in_specs=[in_hbm] * 5 + [pl.BlockSpec(memory_space=pltpu.SMEM)],
        out_specs=pl.BlockSpec(memory_space=pltpu.VMEM),
        scratch_shapes=[
            pltpu.VMEM(src_field.shape, bf16),
            pltpu.VMEM((own_tiles, lanes), i32),
            pltpu.VMEM(packed_counts.shape, i32),
            pltpu.VMEM((1, pairs), i32),
            pltpu.SMEM((pairs,), i32),
            pltpu.VMEM((1, 1, pairs), i32),
            pltpu.VMEM((narrow, 1, pairs), i32),
            pltpu.VMEM((narrow, variables, part, own_tiles * lanes), bf16),
            pltpu.VMEM((own_tiles, variables * levels, lanes), f32),
            pltpu.VMEM((own_tiles, levels, lanes), bf16),
            pltpu.VMEM((own_tiles, variables * levels, lanes), bf16),
            pltpu.VMEM((levels * PITCH, lanes), f32),
            pltpu.VMEM((variables * levels * PITCH, lanes), f32),
            pltpu.VMEM((variables, TB_DEV * part, lanes), f32),
            pltpu.VMEM((narrow, comps, part, pairs, lanes), bf16),
            pltpu.VMEM((4, 3, comps, pairs, lanes), bf16),
            pltpu.VMEM((2, offsets, TB_DEV, 4 * pairs), bf16),
            pltpu.VMEM((part, offsets, comps, TB_DEV, lanes), bf16),
            pltpu.VMEM((part, offsets, comps, TB_DEV, lanes), bf16),
            pltpu.VMEM((offsets, comps, part, TB_DEV, lanes), f32),
            pltpu.VMEM((offsets, comps, part, TB_DEV, lanes), bf16),
            pltpu.VMEM((offsets, comps, part, TB_DEV, lanes), bf16),
            pltpu.SemaphoreType.REGULAR,
            pltpu.SemaphoreType.REGULAR,
            dma((5,)),
            dma((pairs // FETCH,)),
            dma(()),
            dma((narrow,)),
            dma((narrow,)),
            dma((narrow,)),
            dma((narrow,)),
            dma((2, pieces, 4, 3)),
            dma((2, pieces, 4, 3)),
            dma((2, part, offsets)),
            dma((2, part, offsets)),
            dma((2, offsets)),
            dma((2, offsets)),
        ],
        compiler_params=pltpu.CompilerParams(collective_id=0, has_side_effects=True),
    )(
        src_field,
        src_depth.reshape(own_tiles, lanes),
        packed_counts,
        pair_source,
        pair_home.reshape(1, pairs),
        pair_count,
    )


def solution(mesh):
    both = ("wide", "narrow")
    return jax.shard_map(
        functools.partial(per_device, mesh.shape["wide"], mesh.shape["narrow"]),
        mesh=mesh,
        in_specs=(P(None, "narrow", "wide"), P(both), P(both, None, None), P(both), P(both), P(both)),
        out_specs=P(None, "narrow", "wide"),
        check_vma=False,
    )
```

```python
import functools

import jax
import jax.numpy as jnp
from jax import lax
from jax.experimental import pallas as pl
from jax.experimental.pallas import tpu as pltpu
from jax.sharding import PartitionSpec as P

DENOM = 256
REACH = 2
TB_DEV = 64
WET_LIMIT = 0.001
FETCH = 32
PIECES = (((0, 64), (64, 64)), ((0, 32), (32, 32), (64, 64)))
PITCH = 72
MESH = pl.DeviceIdType.MESH

HOP = (1, -1, -1, 1)
FAR = (2, -2, -1, 1)
NEAR = (1, -1, 0, 0)


def kernel(
    wide,
    narrow,
    field_in,
    depth_in,
    counts_in,
    source_in,
    home_in,
    live_in,
    out_ref,
    field_v,
    depth_v,
    counts_v,
    home_v,
    source_s,
    target_v,
    target_r,
    field_r,
    rows_f,
    wet_tiles,
    field_tiles,
    wet_spread,
    field_spread,
    paired,
    terms,
    raw_r,
    select,
    dense_s,
    dense_r,
    partial,
    sums,
    sums_r,
    group_in,
    wide_in,
    local_sem,
    counts_sem,
    self_sem,
    field_ss,
    field_rs,
    target_ss,
    target_rs,
    raw_ss,
    raw_rs,
    dense_ss,
    dense_rs,
    wide_ss,
    wide_rs,
):
    w = lax.axis_index("wide")
    n = lax.axis_index("narrow")
    pairs, half, lanes = counts_v.shape
    own_tiles = wet_tiles.shape[0]
    own_cells = own_tiles * lanes
    variables, part = field_v.shape[0], field_v.shape[1]
    levels = narrow * part
    comps = variables + 1
    offsets = 2 * REACH + 1
    shifts = [o for o in range(offsets) if o != REACH]
    chips = narrow // 2
    core = lax.rem(n, 2)
    chip = n // 2
    other = 1 - core
    twin = 2 * chip + other

    column = lax.rem(w, 8)
    middle = (column // 4) * (1 - lax.rem(column // 2, 2))
    edge = (column // 4) * lax.rem(column // 2, 2) * lax.rem(column, 2)
    urgent = [4 - 4 * middle - edge, 3 - 2 * middle + edge]
    patient = [4 * middle, 1 + 2 * middle]

    def at(hop, c):
        return lax.rem(chip + hop + chips, chips) * 2 + c

    def on_narrow(step):
        return lax.rem(n + step, narrow)

    def on_wide(shift):
        return lax.rem(w + shift + wide, wide)

    def whole(ref, send_sem, recv_sem):
        return pltpu.make_async_remote_copy(
            src_ref=ref,
            dst_ref=ref,
            send_sem=send_sem,
            recv_sem=recv_sem,
            device_id={"narrow": twin},
            device_id_type=MESH,
        )

    first = [
        pltpu.make_async_copy(field_in, field_v, local_sem.at[0]),
        pltpu.make_async_copy(home_in, home_v, local_sem.at[1]),
        pltpu.make_async_copy(depth_in, depth_v, local_sem.at[2]),
        pltpu.make_async_copy(source_in, source_s, local_sem.at[3]),
    ]
    for copy in first:
        copy.start()

    def counts_copy(b):
        rows = pl.ds(b * FETCH, FETCH)
        return pltpu.make_async_copy(counts_in.at[rows], counts_v.at[rows], counts_sem.at[b])

    for b in range(pairs // FETCH):
        counts_copy(b).start()

    barrier = pltpu.get_barrier_semaphore()
    for hop in range(1, chips):
        pl.semaphore_signal(barrier, inc=1, device_id={"narrow": at(hop, 0)}, device_id_type=MESH)
    for o in shifts:
        pl.semaphore_signal(
            barrier, inc=1, device_id={"wide": on_wide(o - REACH), "narrow": at(0, 1)}, device_id_type=MESH
        )

    @pl.when(core == 1)
    def _():
        pl.semaphore_signal(barrier, inc=1, device_id={"narrow": twin}, device_id_type=MESH)

    first[1].wait()
    home = home_v[...]
    slot = lax.broadcasted_iota(jnp.int32, home.shape, 1)
    offset = lax.rem(home // TB_DEV - w + REACH + wide, wide)
    target = jnp.where(slot < live_in[0], offset * TB_DEV + lax.rem(home, TB_DEV), -1)
    target_v[0] = target
    target_r[n] = target
    first[0].wait()

    @pl.when(core == 0)
    def _():
        pl.semaphore_wait(barrier, narrow - 1)
        pl.semaphore_signal(group_in, inc=1, device_id={"narrow": twin}, device_id_type=MESH)

    @pl.when(core == 1)
    def _():
        pl.semaphore_wait(group_in, 1)

    order = [4, 5, 2, 6, 3, 7, 1]

    def field_copy(step, peer, to):
        cells = pl.ds(pl.multiple_of(peer * own_cells, own_cells), own_cells)
        return pltpu.make_async_remote_copy(
            src_ref=field_v.at[:, :, cells],
            dst_ref=field_r.at[to],
            send_sem=field_ss,
            recv_sem=field_rs,
            device_id={"narrow": peer},
            device_id_type=MESH,
        )

    def target_copy(step, peer, to):
        return pltpu.make_async_remote_copy(
            src_ref=target_v,
            dst_ref=target_r.at[pl.ds(to, 1)],
            send_sem=target_ss,
            recv_sem=target_rs,
            device_id={"narrow": peer},
            device_id_type=MESH,
        )

    for step in order:
        field_copy(step, on_narrow(step), n).start()
    for step in order:
        target_copy(step, on_narrow(step), n).start()
    own_span = pl.ds(pl.multiple_of(n * own_cells, own_cells), own_cells)
    own_field = pltpu.make_async_copy(field_v.at[:, :, own_span], field_r.at[n], self_sem)
    own_field.start()

    def terms_of(lo, size, stored, spread):
        comps_rows = stored.shape[1]

        def one_pair(i, carry):
            p = lo + i
            words = counts_v[p]
            low = (words & 65535).astype(jnp.float32) * (1.0 / DENOM)
            high = lax.shift_right_logical(words, 16).astype(jnp.float32) * (1.0 / DENOM)
            weight = jnp.concatenate([low.astype(jnp.bfloat16), high.astype(jnp.bfloat16)], axis=0)
            term = lax.dot_general(
                stored[source_s[p]], weight, (((1,), (1,)), ((), ())), preferred_element_type=jnp.float32
            )
            spread[pl.ds(i, comps_rows, stride=PITCH), :] = term
            return carry

        lax.fori_loop(0, size, one_pair, 0, unroll=32)

    def store_terms(lo, size, c, r0, spread):
        for l in range(levels):
            r = r0 + l
            block = spread[r * PITCH : r * PITCH + size, :].astype(jnp.bfloat16)
            terms[l // part, c, l % part, lo : lo + size, :] = block

    spans = (slice(0, 1), slice(1, comps))

    def raw_copy(g, k, role, t):
        lo, size = PIECES[g][k] if k is not None else (0, pairs)
        if t < 2:
            peer, data, mine = at(HOP[role], t), at(FAR[role], t), core
        else:
            peer, data, mine = twin, at(NEAR[role], other), 2
        return pltpu.make_async_remote_copy(
            src_ref=terms.at[data, spans[g], role % part, lo : lo + size],
            dst_ref=raw_r.at[role, mine, spans[g], lo : lo + size],
            send_sem=raw_ss,
            recv_sem=raw_rs.at[g, role // 2],
            device_id={"narrow": peer},
            device_id_type=MESH,
        )

    def send_raw(g, k, roles):
        for t in range(3):
            for role in roles:
                raw_copy(g, k, role, t).start()

    def wait_raw(g, roles):
        lo, hi = roles[0], roles[-1] + 1
        whole(raw_r.at[lo:hi, :, spans[g]], raw_ss, raw_rs.at[g, lo // 2]).wait_recv()

    first[2].wait()
    first[3].wait()
    level_ids = lax.broadcasted_iota(jnp.int32, (levels, lanes), 0)
    for s in range(own_tiles):
        wet = level_ids < depth_v[s : s + 1, :]
        wet_tiles[s] = jnp.where(wet, 1.0, 0.0).astype(jnp.bfloat16)
    for k, (lo, size) in enumerate(PIECES[0]):
        for b in range(lo // FETCH, (lo + size) // FETCH):
            counts_copy(b).wait()
        terms_of(lo, size, wet_tiles, wet_spread)
        store_terms(lo, size, 0, 0, wet_spread)
        send_raw(0, k, (0, 1))
        send_raw(0, k, (2, 3))

    own_field.wait()
    whole(field_r.at[1:], field_ss, field_rs).wait_recv()
    for m in range(narrow):
        for v in range(variables):
            for s in range(own_tiles):
                piece = field_r[m, v, :, s * lanes : (s + 1) * lanes]
                rows_f[s, v * levels + m * part : v * levels + (m + 1) * part, :] = piece.astype(jnp.float32)
    for s in range(own_tiles):
        wet = level_ids < depth_v[s : s + 1, :]
        for v in range(variables):
            rows = rows_f[s, v * levels : (v + 1) * levels, :]
            field_tiles[s, v * levels : (v + 1) * levels, :] = jnp.where(wet, rows, 0.0).astype(jnp.bfloat16)

    for k, (lo, size) in enumerate(PIECES[1]):
        terms_of(lo, size, field_tiles, field_spread)
        for v in range(variables):
            store_terms(lo, size, v + 1, v * levels, field_spread)
        send_raw(1, k, (0, 1))

    whole(target_r.at[1:], target_ss, target_rs).wait_recv()
    for side, hop in enumerate((-1, 1)):
        for q, m in enumerate((at(hop, 0), at(hop, 1), twin, n)):
            row = target_r[m]
            for o in range(offsets):
                ids = o * TB_DEV + lax.broadcasted_iota(jnp.int32, (TB_DEV, pairs), 0)
                hit = jnp.where(ids == row, 1.0, 0.0).astype(jnp.bfloat16)
                select[side, o, :, q * pairs : (q + 1) * pairs] = hit

    def gathered(g, role):
        mine = at(NEAR[role], core)
        columns = []
        for c in range(spans[g].start, spans[g].stop):
            columns.append(
                jnp.concatenate([raw_r[role, t, c] for t in range(3)] + [terms[mine, c, role % part]], axis=0)
            )
        return jnp.concatenate(columns, axis=1) if len(columns) > 1 else columns[0]

    def add_up(role, o, received):
        side = 0 if HOP[role] == 1 else 1
        return jnp.dot(select[side, o], received, preferred_element_type=jnp.float32)

    def dense_copy(g, j, o, peer):
        return pltpu.make_async_remote_copy(
            src_ref=dense_s.at[j, o, spans[g]],
            dst_ref=dense_r.at[j, o, spans[g]],
            send_sem=dense_ss,
            recv_sem=dense_rs.at[g, o],
            device_id={"narrow": peer},
            device_id_type=MESH,
        )

    def relay(g, o, received):
        for role in (0, 1):
            total = add_up(role, o, received[role])
            for i, c in enumerate(range(spans[g].start, spans[g].stop)):
                dense_s[role, o, c] = total[:, i * lanes : (i + 1) * lanes].astype(jnp.bfloat16)

    def pass_on(g, o):
        for role in (0, 1):
            dense_copy(g, role, o, at(HOP[role], core)).start()

    def gather_own(g, offs):
        received = [gathered(g, role) for role in (2, 3)]
        for o in offs:
            for role in (2, 3):
                total = add_up(role, o, received[role - 2])
                for i, c in enumerate(range(spans[g].start, spans[g].stop)):
                    partial[o, c, role % part] = total[:, i * lanes : (i + 1) * lanes]

    def wide_copy(g, o, to):
        return pltpu.make_async_remote_copy(
            src_ref=sums.at[o, spans[g]],
            dst_ref=sums_r.at[o, spans[g]],
            send_sem=wide_ss,
            recv_sem=wide_rs.at[g],
            device_id={"wide": to},
            device_id_type=MESH,
        )

    def finish(g, o, leaves):
        whole(dense_r.at[:, o, spans[g]], dense_ss, dense_rs.at[g, o]).wait_recv()
        for c in range(spans[g].start, spans[g].stop):
            for j in range(part):
                total = partial[o, c, j] + dense_r[j, o, c].astype(jnp.float32)
                if leaves:
                    sums[o, c, j] = total.astype(jnp.bfloat16)
                else:
                    partial[o, c, j] = total
        if leaves:
            wide_copy(g, o, on_wide(o - REACH)).start()

    every = urgent + patient + [REACH]
    wait_raw(0, (0, 1))
    received = [gathered(0, role) for role in (0, 1)]
    for o in urgent:
        relay(0, o, received)
        pass_on(0, o)
    send_raw(1, None, (2, 3))
    for o in patient + [REACH]:
        relay(0, o, received)
    wait_raw(0, (2, 3))
    gather_own(0, every)

    wait_raw(1, (0, 1))
    received = [gathered(1, role) for role in (0, 1)]
    for o in urgent:
        relay(1, o, received)
        pass_on(1, o)
    for o in patient + [REACH]:
        pass_on(0, o)
    for o in patient + [REACH]:
        relay(1, o, received)
        pass_on(1, o)

    @pl.when(core == 1)
    def _():
        pl.semaphore_wait(barrier, 2 * len(shifts))
        pl.semaphore_signal(wide_in, inc=1, device_id={"narrow": twin}, device_id_type=MESH)

    @pl.when(core == 0)
    def _():
        pl.semaphore_wait(wide_in, 1)

    for o in urgent:
        finish(0, o, True)
    wait_raw(1, (2, 3))
    gather_own(1, every)
    for o in urgent:
        finish(1, o, True)
    for o in patient:
        finish(0, o, True)
    for o in patient:
        finish(1, o, True)
    for g in range(2):
        finish(g, REACH, False)

    own_part = own_cells * (narrow - 1)
    whole(field_v.at[:, :, :own_part], field_ss, field_rs).wait_send()
    whole(target_r.at[1:], target_ss, target_rs).wait_send()
    whole(terms.at[2:], raw_ss, raw_rs.at[0, 0]).wait_send()
    whole(dense_s, dense_ss, dense_rs.at[0, 0]).wait_send()

    def total_of(c):
        total = partial[REACH, c]
        for o in shifts:
            total = total + sums_r[o, c].astype(jnp.float32)
        return total

    whole(sums_r.at[1:, spans[0]], wide_ss, wide_rs.at[0]).wait_recv()
    wet_total = total_of(0)
    covered = wet_total > WET_LIMIT
    safe = jnp.where(covered, wet_total, 1.0)
    whole(sums_r.at[1:, spans[1]], wide_ss, wide_rs.at[1]).wait_recv()
    for v in range(variables):
        result = jnp.where(covered, total_of(v + 1) / safe, 0.0)
        for j in range(part):
            paired[v, pl.ds(j, TB_DEV, stride=part), :] = result[j]
        for t in range(TB_DEV):
            out_ref[v, :, t * lanes : (t + 1) * lanes] = paired[v, t * part : (t + 1) * part, :].astype(out_ref.dtype)

    whole(sums.at[1:], wide_ss, wide_rs.at[0]).wait_send()


def per_device(wide, narrow, src_field, src_depth, packed_counts, pair_source, pair_home, pair_count):
    variables, part, _ = src_field.shape
    pairs, _, lanes = packed_counts.shape
    own_tiles = src_depth.shape[0] // lanes
    levels = narrow * part
    comps = variables + 1
    offsets = 2 * REACH + 1
    dma = pltpu.SemaphoreType.DMA
    bf16, f32, i32 = jnp.bfloat16, jnp.float32, jnp.int32
    in_hbm = pl.BlockSpec(memory_space=pltpu.HBM)
    return pl.pallas_call(
        functools.partial(kernel, wide, narrow),
        out_shape=pltpu.VMEM((variables, part, TB_DEV * lanes), bf16),
        in_specs=[in_hbm] * 5 + [pl.BlockSpec(memory_space=pltpu.SMEM)],
        out_specs=pl.BlockSpec(memory_space=pltpu.VMEM),
        scratch_shapes=[
            pltpu.VMEM(src_field.shape, bf16),
            pltpu.VMEM((own_tiles, lanes), i32),
            pltpu.VMEM(packed_counts.shape, i32),
            pltpu.VMEM((1, pairs), i32),
            pltpu.SMEM((pairs,), i32),
            pltpu.VMEM((1, 1, pairs), i32),
            pltpu.VMEM((narrow, 1, pairs), i32),
            pltpu.VMEM((narrow, variables, part, own_tiles * lanes), bf16),
            pltpu.VMEM((own_tiles, variables * levels, lanes), f32),
            pltpu.VMEM((own_tiles, levels, lanes), bf16),
            pltpu.VMEM((own_tiles, variables * levels, lanes), bf16),
            pltpu.VMEM((levels * PITCH, lanes), f32),
            pltpu.VMEM((variables * levels * PITCH, lanes), f32),
            pltpu.VMEM((variables, TB_DEV * part, lanes), f32),
            pltpu.VMEM((narrow, comps, part, pairs, lanes), bf16),
            pltpu.VMEM((4, 3, comps, pairs, lanes), bf16),
            pltpu.VMEM((2, offsets, TB_DEV, 4 * pairs), bf16),
            pltpu.VMEM((part, offsets, comps, TB_DEV, lanes), bf16),
            pltpu.VMEM((part, offsets, comps, TB_DEV, lanes), bf16),
            pltpu.VMEM((offsets, comps, part, TB_DEV, lanes), f32),
            pltpu.VMEM((offsets, comps, part, TB_DEV, lanes), bf16),
            pltpu.VMEM((offsets, comps, part, TB_DEV, lanes), bf16),
            pltpu.SemaphoreType.REGULAR,
            pltpu.SemaphoreType.REGULAR,
            dma((4,)),
            dma((pairs // FETCH,)),
            dma(()),
            dma(()),
            dma(()),
            dma(()),
            dma(()),
            dma(()),
            dma((2, 2)),
            dma(()),
            dma((2, offsets)),
            dma(()),
            dma((2,)),
        ],
        compiler_params=pltpu.CompilerParams(collective_id=0, has_side_effects=True),
    )(
        src_field,
        src_depth.reshape(own_tiles, lanes),
        packed_counts,
        pair_source,
        pair_home.reshape(1, pairs),
        pair_count,
    )


def solution(mesh):
    both = ("wide", "narrow")
    return jax.shard_map(
        functools.partial(per_device, mesh.shape["wide"], mesh.shape["narrow"]),
        mesh=mesh,
        in_specs=(P(None, "narrow", "wide"), P(both), P(both, None, None), P(both), P(both), P(both)),
        out_specs=P(None, "narrow", "wide"),
        check_vma=False,
    )
```

```python
import functools

import jax
import jax.numpy as jnp
from jax import lax
from jax.experimental import pallas as pl
from jax.experimental.pallas import tpu as pltpu
from jax.sharding import PartitionSpec as P

DENOM = 256
REACH = 2
TB_DEV = 64
WET_LIMIT = 0.001
FETCH = 32
WET_PIECES = ((0, 64), (64, 64))
PIECES = ((0, 32), (32, 32), (64, 64))
PITCH = 72
MESH = pl.DeviceIdType.MESH

HOP = (1, -1, -1, 1)
FAR = (2, -2, -1, 1)
NEAR = (1, -1, 0, 0)


def kernel(
    wide,
    narrow,
    field_in,
    depth_in,
    counts_in,
    source_in,
    home_in,
    live_in,
    out_ref,
    field_v,
    depth_v,
    counts_v,
    home_v,
    source_s,
    target_v,
    target_r,
    field_r,
    rows_f,
    wet_tiles,
    field_tiles,
    wet_spread,
    field_spread,
    paired,
    terms,
    raw_r,
    select,
    dense_s,
    dense_r,
    partial,
    sums,
    sums_r,
    group_in,
    wide_in,
    local_sem,
    counts_sem,
    self_sem,
    field_ss,
    field_rs,
    target_ss,
    target_rs,
    raw_ss,
    raw_rs,
    dense_ss,
    dense_rs,
    wide_ss,
    wide_rs,
):
    w = lax.axis_index("wide")
    n = lax.axis_index("narrow")
    pairs, half, lanes = counts_v.shape
    own_tiles = wet_tiles.shape[0]
    own_cells = own_tiles * lanes
    variables, part = field_v.shape[0], field_v.shape[1]
    levels = narrow * part
    comps = variables + 1
    offsets = 2 * REACH + 1
    shifts = [o for o in range(offsets) if o != REACH]
    chips = narrow // 2
    core = lax.rem(n, 2)
    chip = n // 2
    other = 1 - core
    twin = 2 * chip + other

    column = lax.rem(w, 8)
    middle = (column // 4) * (1 - lax.rem(column // 2, 2))
    edge = (column // 4) * lax.rem(column // 2, 2) * lax.rem(column, 2)
    urgent = [4 - 4 * middle - edge, 3 - 2 * middle + edge]
    patient = [4 * middle, 1 + 2 * middle]

    def at(hop, c):
        return lax.rem(chip + hop + chips, chips) * 2 + c

    def on_narrow(step):
        return lax.rem(n + step, narrow)

    def on_wide(shift):
        return lax.rem(w + shift + wide, wide)

    def whole(ref, send_sem, recv_sem):
        return pltpu.make_async_remote_copy(
            src_ref=ref,
            dst_ref=ref,
            send_sem=send_sem,
            recv_sem=recv_sem,
            device_id={"narrow": twin},
            device_id_type=MESH,
        )

    first = [
        pltpu.make_async_copy(field_in, field_v, local_sem.at[0]),
        pltpu.make_async_copy(home_in, home_v, local_sem.at[1]),
        pltpu.make_async_copy(depth_in, depth_v, local_sem.at[2]),
        pltpu.make_async_copy(source_in, source_s, local_sem.at[3]),
    ]
    for copy in first:
        copy.start()

    def counts_copy(b):
        rows = pl.ds(b * FETCH, FETCH)
        return pltpu.make_async_copy(counts_in.at[rows], counts_v.at[rows], counts_sem.at[b])

    for b in range(pairs // FETCH):
        counts_copy(b).start()

    barrier = pltpu.get_barrier_semaphore()
    for hop in range(1, chips):
        pl.semaphore_signal(barrier, inc=1, device_id={"narrow": at(hop, 0)}, device_id_type=MESH)
    for o in shifts:
        pl.semaphore_signal(
            barrier, inc=1, device_id={"wide": on_wide(o - REACH), "narrow": at(0, 1)}, device_id_type=MESH
        )

    @pl.when(core == 1)
    def _():
        pl.semaphore_signal(barrier, inc=1, device_id={"narrow": twin}, device_id_type=MESH)

    first[1].wait()
    home = home_v[...]
    slot = lax.broadcasted_iota(jnp.int32, home.shape, 1)
    offset = lax.rem(home // TB_DEV - w + REACH + wide, wide)
    target = jnp.where(slot < live_in[0], offset * TB_DEV + lax.rem(home, TB_DEV), -1)
    target_v[0] = target
    target_r[n] = target
    first[0].wait()

    @pl.when(core == 0)
    def _():
        pl.semaphore_wait(barrier, narrow - 1)
        pl.semaphore_signal(group_in, inc=1, device_id={"narrow": twin}, device_id_type=MESH)

    @pl.when(core == 1)
    def _():
        pl.semaphore_wait(group_in, 1)

    order = [4, 5, 2, 6, 3, 7, 1]

    def field_copy(step, peer, to):
        cells = pl.ds(pl.multiple_of(peer * own_cells, own_cells), own_cells)
        return pltpu.make_async_remote_copy(
            src_ref=field_v.at[:, :, cells],
            dst_ref=field_r.at[to],
            send_sem=field_ss,
            recv_sem=field_rs,
            device_id={"narrow": peer},
            device_id_type=MESH,
        )

    def target_copy(step, peer, to):
        return pltpu.make_async_remote_copy(
            src_ref=target_v,
            dst_ref=target_r.at[pl.ds(to, 1)],
            send_sem=target_ss,
            recv_sem=target_rs,
            device_id={"narrow": peer},
            device_id_type=MESH,
        )

    for step in order:
        target_copy(step, on_narrow(step), n).start()
    for step in order:
        field_copy(step, on_narrow(step), n).start()
    own_span = pl.ds(pl.multiple_of(n * own_cells, own_cells), own_cells)
    own_field = pltpu.make_async_copy(field_v.at[:, :, own_span], field_r.at[n], self_sem)
    own_field.start()

    def terms_of(lo, size, stored, spread):
        comps_rows = stored.shape[1]

        def one_pair(i, carry):
            p = lo + i
            words = counts_v[p]
            low = (words & 65535).astype(jnp.float32) * (1.0 / DENOM)
            high = lax.shift_right_logical(words, 16).astype(jnp.float32) * (1.0 / DENOM)
            weight = jnp.concatenate([low.astype(jnp.bfloat16), high.astype(jnp.bfloat16)], axis=0)
            term = lax.dot_general(
                stored[source_s[p]], weight, (((1,), (1,)), ((), ())), preferred_element_type=jnp.float32
            )
            spread[pl.ds(i, comps_rows, stride=PITCH), :] = term
            return carry

        lax.fori_loop(0, size, one_pair, 0, unroll=32)

    def store_terms(lo, size, c, r0, spread):
        for l in range(levels):
            r = r0 + l
            block = spread[r * PITCH : r * PITCH + size, :].astype(jnp.bfloat16)
            terms[l // part, c, l % part, lo : lo + size, :] = block

    spans = [slice(c, c + 1) for c in range(comps)]
    fields = range(1, comps)

    def raw_copy(g, k, role, t):
        lo, size = (0, pairs) if k is None else (PIECES if g else WET_PIECES)[k]
        if t < 2:
            peer, data, mine = at(HOP[role], t), at(FAR[role], t), core
        else:
            peer, data, mine = twin, at(NEAR[role], other), 2
        return pltpu.make_async_remote_copy(
            src_ref=terms.at[data, spans[g], role % part, lo : lo + size],
            dst_ref=raw_r.at[role, mine, spans[g], lo : lo + size],
            send_sem=raw_ss,
            recv_sem=raw_rs.at[g, role // 2],
            device_id={"narrow": peer},
            device_id_type=MESH,
        )

    def send_raw(g, k, roles):
        for t in range(3):
            for role in roles:
                raw_copy(g, k, role, t).start()

    def wait_raw(g, roles):
        lo, hi = roles[0], roles[-1] + 1
        whole(raw_r.at[lo:hi, :, spans[g]], raw_ss, raw_rs.at[g, lo // 2]).wait_recv()

    first[2].wait()
    first[3].wait()
    level_ids = lax.broadcasted_iota(jnp.int32, (levels, lanes), 0)
    for s in range(own_tiles):
        wet = level_ids < depth_v[s : s + 1, :]
        wet_tiles[s] = jnp.where(wet, 1.0, 0.0).astype(jnp.bfloat16)
    for k, (lo, size) in enumerate(WET_PIECES):
        for b in range(lo // FETCH, (lo + size) // FETCH):
            counts_copy(b).wait()
        terms_of(lo, size, wet_tiles, wet_spread)
        store_terms(lo, size, 0, 0, wet_spread)
        send_raw(0, k, (0, 1))
        send_raw(0, k, (2, 3))

    whole(target_r.at[1:], target_ss, target_rs).wait_recv()
    for side, hop in enumerate((-1, 1)):
        for q, m in enumerate((at(hop, 0), at(hop, 1), twin, n)):
            row = target_r[m]
            for o in range(offsets):
                ids = o * TB_DEV + lax.broadcasted_iota(jnp.int32, (TB_DEV, pairs), 0)
                hit = jnp.where(ids == row, 1.0, 0.0).astype(jnp.bfloat16)
                select[side, o, :, q * pairs : (q + 1) * pairs] = hit

    own_field.wait()
    whole(field_r.at[1:], field_ss, field_rs).wait_recv()
    for m in range(narrow):
        for v in range(variables):
            for s in range(own_tiles):
                piece = field_r[m, v, :, s * lanes : (s + 1) * lanes]
                rows_f[s, v * levels + m * part : v * levels + (m + 1) * part, :] = piece.astype(jnp.float32)
    for s in range(own_tiles):
        wet = level_ids < depth_v[s : s + 1, :]
        for v in range(variables):
            rows = rows_f[s, v * levels : (v + 1) * levels, :]
            field_tiles[s, v * levels : (v + 1) * levels, :] = jnp.where(wet, rows, 0.0).astype(jnp.bfloat16)

    for k, (lo, size) in enumerate(PIECES):
        terms_of(lo, size, field_tiles, field_spread)
        for v in range(variables):
            store_terms(lo, size, v + 1, v * levels, field_spread)
        for g in fields:
            send_raw(g, k, (0, 1))

    def gathered(g, role):
        mine = at(NEAR[role], core)
        columns = []
        for c in range(spans[g].start, spans[g].stop):
            columns.append(
                jnp.concatenate([raw_r[role, t, c] for t in range(3)] + [terms[mine, c, role % part]], axis=0)
            )
        return jnp.concatenate(columns, axis=1) if len(columns) > 1 else columns[0]

    def add_up(role, o, received):
        side = 0 if HOP[role] == 1 else 1
        return jnp.dot(select[side, o], received, preferred_element_type=jnp.float32)

    def dense_copy(g, j, o, peer):
        return pltpu.make_async_remote_copy(
            src_ref=dense_s.at[j, o, spans[g]],
            dst_ref=dense_r.at[j, o, spans[g]],
            send_sem=dense_ss,
            recv_sem=dense_rs.at[g, o],
            device_id={"narrow": peer},
            device_id_type=MESH,
        )

    def relay(g, o, received):
        for role in (0, 1):
            total = add_up(role, o, received[role])
            for i, c in enumerate(range(spans[g].start, spans[g].stop)):
                dense_s[role, o, c] = total[:, i * lanes : (i + 1) * lanes].astype(jnp.bfloat16)

    def pass_on(g, o):
        for role in (0, 1):
            dense_copy(g, role, o, at(HOP[role], core)).start()

    def gather_own(g, offs):
        received = [gathered(g, role) for role in (2, 3)]
        for o in offs:
            for role in (2, 3):
                total = add_up(role, o, received[role - 2])
                for i, c in enumerate(range(spans[g].start, spans[g].stop)):
                    partial[o, c, role % part] = total[:, i * lanes : (i + 1) * lanes]

    def wide_copy(g, o, to):
        return pltpu.make_async_remote_copy(
            src_ref=sums.at[o, spans[g]],
            dst_ref=sums_r.at[o, spans[g]],
            send_sem=wide_ss,
            recv_sem=wide_rs.at[g],
            device_id={"wide": to},
            device_id_type=MESH,
        )

    def finish(g, o, leaves):
        whole(dense_r.at[:, o, spans[g]], dense_ss, dense_rs.at[g, o]).wait_recv()
        for c in range(spans[g].start, spans[g].stop):
            for j in range(part):
                total = partial[o, c, j] + dense_r[j, o, c].astype(jnp.float32)
                if leaves:
                    sums[o, c, j] = total.astype(jnp.bfloat16)
                else:
                    partial[o, c, j] = total
        if leaves:
            wide_copy(g, o, on_wide(o - REACH)).start()

    def relays(g, offs, received):
        for o in offs:
            relay(g, o, received)
            pass_on(g, o)

    rest = patient + [REACH]
    received = []
    for g in range(comps):
        wait_raw(g, (0, 1))
        received.append([gathered(g, role) for role in (0, 1)])
        relays(g, urgent, received[g])
        if g < variables:
            send_raw(g + 1, None, (2, 3))
        if g == 0:
            wait_raw(0, (2, 3))
            gather_own(0, urgent + rest)

    @pl.when(core == 1)
    def _():
        pl.semaphore_wait(barrier, 2 * len(shifts))
        pl.semaphore_signal(wide_in, inc=1, device_id={"narrow": twin}, device_id_type=MESH)

    @pl.when(core == 0)
    def _():
        pl.semaphore_wait(wide_in, 1)

    for o in urgent:
        finish(0, o, True)
    for g in range(comps):
        relays(g, rest, received[g])
    for g in fields:
        wait_raw(g, (2, 3))
        gather_own(g, urgent)
        for o in urgent:
            finish(g, o, True)
        gather_own(g, rest)
    for g in range(comps):
        for o in patient:
            finish(g, o, True)
    for g in range(comps):
        finish(g, REACH, False)

    own_part = own_cells * (narrow - 1)
    whole(field_v.at[:, :, :own_part], field_ss, field_rs).wait_send()
    whole(target_r.at[1:], target_ss, target_rs).wait_send()
    whole(terms.at[2:], raw_ss, raw_rs.at[0, 0]).wait_send()
    whole(dense_s, dense_ss, dense_rs.at[0, 0]).wait_send()

    def total_of(c):
        total = partial[REACH, c]
        for o in shifts:
            total = total + sums_r[o, c].astype(jnp.float32)
        return total

    whole(sums_r.at[1:, spans[0]], wide_ss, wide_rs.at[0]).wait_recv()
    wet_total = total_of(0)
    covered = wet_total > WET_LIMIT
    safe = jnp.where(covered, wet_total, 1.0)
    for v in range(variables):
        whole(sums_r.at[1:, spans[v + 1]], wide_ss, wide_rs.at[v + 1]).wait_recv()
        result = jnp.where(covered, total_of(v + 1) / safe, 0.0)
        for j in range(part):
            paired[v, pl.ds(j, TB_DEV, stride=part), :] = result[j]
        for t in range(TB_DEV):
            out_ref[v, :, t * lanes : (t + 1) * lanes] = paired[v, t * part : (t + 1) * part, :].astype(out_ref.dtype)

    whole(sums.at[1:], wide_ss, wide_rs.at[0]).wait_send()


def per_device(wide, narrow, src_field, src_depth, packed_counts, pair_source, pair_home, pair_count):
    variables, part, _ = src_field.shape
    pairs, _, lanes = packed_counts.shape
    own_tiles = src_depth.shape[0] // lanes
    levels = narrow * part
    comps = variables + 1
    offsets = 2 * REACH + 1
    dma = pltpu.SemaphoreType.DMA
    bf16, f32, i32 = jnp.bfloat16, jnp.float32, jnp.int32
    in_hbm = pl.BlockSpec(memory_space=pltpu.HBM)
    return pl.pallas_call(
        functools.partial(kernel, wide, narrow),
        out_shape=pltpu.VMEM((variables, part, TB_DEV * lanes), bf16),
        in_specs=[in_hbm] * 5 + [pl.BlockSpec(memory_space=pltpu.SMEM)],
        out_specs=pl.BlockSpec(memory_space=pltpu.VMEM),
        scratch_shapes=[
            pltpu.VMEM(src_field.shape, bf16),
            pltpu.VMEM((own_tiles, lanes), i32),
            pltpu.VMEM(packed_counts.shape, i32),
            pltpu.VMEM((1, pairs), i32),
            pltpu.SMEM((pairs,), i32),
            pltpu.VMEM((1, 1, pairs), i32),
            pltpu.VMEM((narrow, 1, pairs), i32),
            pltpu.VMEM((narrow, variables, part, own_tiles * lanes), bf16),
            pltpu.VMEM((own_tiles, variables * levels, lanes), f32),
            pltpu.VMEM((own_tiles, levels, lanes), bf16),
            pltpu.VMEM((own_tiles, variables * levels, lanes), bf16),
            pltpu.VMEM((levels * PITCH, lanes), f32),
            pltpu.VMEM((variables * levels * PITCH, lanes), f32),
            pltpu.VMEM((variables, TB_DEV * part, lanes), f32),
            pltpu.VMEM((narrow, comps, part, pairs, lanes), bf16),
            pltpu.VMEM((4, 3, comps, pairs, lanes), bf16),
            pltpu.VMEM((2, offsets, TB_DEV, 4 * pairs), bf16),
            pltpu.VMEM((part, offsets, comps, TB_DEV, lanes), bf16),
            pltpu.VMEM((part, offsets, comps, TB_DEV, lanes), bf16),
            pltpu.VMEM((offsets, comps, part, TB_DEV, lanes), f32),
            pltpu.VMEM((offsets, comps, part, TB_DEV, lanes), bf16),
            pltpu.VMEM((offsets, comps, part, TB_DEV, lanes), bf16),
            pltpu.SemaphoreType.REGULAR,
            pltpu.SemaphoreType.REGULAR,
            dma((4,)),
            dma((pairs // FETCH,)),
            dma(()),
            dma(()),
            dma(()),
            dma(()),
            dma(()),
            dma(()),
            dma((comps, 2)),
            dma(()),
            dma((comps, offsets)),
            dma(()),
            dma((comps,)),
        ],
        compiler_params=pltpu.CompilerParams(collective_id=0, has_side_effects=True),
    )(
        src_field,
        src_depth.reshape(own_tiles, lanes),
        packed_counts,
        pair_source,
        pair_home.reshape(1, pairs),
        pair_count,
    )


def solution(mesh):
    both = ("wide", "narrow")
    return jax.shard_map(
        functools.partial(per_device, mesh.shape["wide"], mesh.shape["narrow"]),
        mesh=mesh,
        in_specs=(P(None, "narrow", "wide"), P(both), P(both, None, None), P(both), P(both), P(both)),
        out_specs=P(None, "narrow", "wide"),
        check_vma=False,
    )
```

```python
import functools

import jax
import jax.numpy as jnp
from jax import lax
from jax.experimental import pallas as pl
from jax.experimental.pallas import tpu as pltpu
from jax.sharding import PartitionSpec as P

DENOM = 256
REACH = 2
TB_DEV = 64
WET_LIMIT = 0.001
FETCH = 32
WET_PIECES = ((0, 64), (64, 64))
PIECES = ((0, 32), (32, 32), (64, 32), (96, 32))
PITCH = 72
MESH = pl.DeviceIdType.MESH

HOP = (1, -1, -1, 1)
FAR = (2, -2, -1, 1)
NEAR = (1, -1, 0, 0)


def kernel(
    wide,
    narrow,
    field_in,
    depth_in,
    counts_in,
    source_in,
    home_in,
    live_in,
    out_ref,
    field_v,
    depth_v,
    counts_v,
    home_v,
    source_s,
    target_v,
    target_r,
    field_r,
    rows_f,
    wet_tiles,
    field_tiles,
    wet_spread,
    field_spread,
    paired,
    terms,
    raw_r,
    select,
    dense_s,
    dense_r,
    partial,
    sums,
    sums_r,
    group_in,
    wide_in,
    local_sem,
    counts_sem,
    self_sem,
    field_ss,
    field_rs,
    target_ss,
    target_rs,
    raw_ss,
    raw_rs,
    dense_ss,
    dense_rs,
    wide_ss,
    wide_rs,
):
    w = lax.axis_index("wide")
    n = lax.axis_index("narrow")
    pairs, half, lanes = counts_v.shape
    own_tiles = wet_tiles.shape[0]
    own_cells = own_tiles * lanes
    variables, part = field_v.shape[0], field_v.shape[1]
    levels = narrow * part
    comps = variables + 1
    offsets = 2 * REACH + 1
    shifts = [o for o in range(offsets) if o != REACH]
    chips = narrow // 2
    core = lax.rem(n, 2)
    chip = n // 2
    other = 1 - core
    twin = 2 * chip + other

    column = lax.rem(w, 8)
    middle = (column // 4) * (1 - lax.rem(column // 2, 2))
    edge = (column // 4) * lax.rem(column // 2, 2) * lax.rem(column, 2)
    urgent = [4 - 4 * middle - edge, 3 - 2 * middle + edge]
    patient = [4 * middle, 1 + 2 * middle]

    def at(hop, c):
        return lax.rem(chip + hop + chips, chips) * 2 + c

    def on_narrow(step):
        return lax.rem(n + step, narrow)

    def on_wide(shift):
        return lax.rem(w + shift + wide, wide)

    def whole(ref, send_sem, recv_sem):
        return pltpu.make_async_remote_copy(
            src_ref=ref,
            dst_ref=ref,
            send_sem=send_sem,
            recv_sem=recv_sem,
            device_id={"narrow": twin},
            device_id_type=MESH,
        )

    first = [
        pltpu.make_async_copy(field_in, field_v, local_sem.at[0]),
        pltpu.make_async_copy(home_in, home_v, local_sem.at[1]),
        pltpu.make_async_copy(depth_in, depth_v, local_sem.at[2]),
        pltpu.make_async_copy(source_in, source_s, local_sem.at[3]),
    ]
    for copy in first:
        copy.start()

    def counts_copy(b):
        rows = pl.ds(b * FETCH, FETCH)
        return pltpu.make_async_copy(counts_in.at[rows], counts_v.at[rows], counts_sem.at[b])

    for b in range(pairs // FETCH):
        counts_copy(b).start()

    barrier = pltpu.get_barrier_semaphore()
    for hop in range(1, chips):
        pl.semaphore_signal(barrier, inc=1, device_id={"narrow": at(hop, 0)}, device_id_type=MESH)
    for o in shifts:
        pl.semaphore_signal(
            barrier, inc=1, device_id={"wide": on_wide(o - REACH), "narrow": at(0, 1)}, device_id_type=MESH
        )

    @pl.when(core == 1)
    def _():
        pl.semaphore_signal(barrier, inc=1, device_id={"narrow": twin}, device_id_type=MESH)

    first[1].wait()
    home = home_v[...]
    slot = lax.broadcasted_iota(jnp.int32, home.shape, 1)
    offset = lax.rem(home // TB_DEV - w + REACH + wide, wide)
    target = jnp.where(slot < live_in[0], offset * TB_DEV + lax.rem(home, TB_DEV), -1)
    target_v[0] = target
    target_r[n] = target
    first[0].wait()

    @pl.when(core == 0)
    def _():
        pl.semaphore_wait(barrier, narrow - 1)
        pl.semaphore_signal(group_in, inc=1, device_id={"narrow": twin}, device_id_type=MESH)

    @pl.when(core == 1)
    def _():
        pl.semaphore_wait(group_in, 1)

    order = [4, 5, 2, 6, 3, 7, 1]

    def field_copy(step, peer, to):
        cells = pl.ds(pl.multiple_of(peer * own_cells, own_cells), own_cells)
        return pltpu.make_async_remote_copy(
            src_ref=field_v.at[:, :, cells],
            dst_ref=field_r.at[to],
            send_sem=field_ss,
            recv_sem=field_rs,
            device_id={"narrow": peer},
            device_id_type=MESH,
        )

    def target_copy(step, peer, to):
        return pltpu.make_async_remote_copy(
            src_ref=target_v,
            dst_ref=target_r.at[pl.ds(to, 1)],
            send_sem=target_ss,
            recv_sem=target_rs,
            device_id={"narrow": peer},
            device_id_type=MESH,
        )

    for step in order:
        target_copy(step, on_narrow(step), n).start()
    for step in order:
        field_copy(step, on_narrow(step), n).start()
    own_span = pl.ds(pl.multiple_of(n * own_cells, own_cells), own_cells)
    own_field = pltpu.make_async_copy(field_v.at[:, :, own_span], field_r.at[n], self_sem)
    own_field.start()

    def terms_of(lo, size, stored, spread):
        comps_rows = stored.shape[1]

        def one_pair(i, carry):
            p = lo + i
            words = counts_v[p]
            low = (words & 65535).astype(jnp.float32) * (1.0 / DENOM)
            high = lax.shift_right_logical(words, 16).astype(jnp.float32) * (1.0 / DENOM)
            weight = jnp.concatenate([low.astype(jnp.bfloat16), high.astype(jnp.bfloat16)], axis=0)
            term = lax.dot_general(
                stored[source_s[p]], weight, (((1,), (1,)), ((), ())), preferred_element_type=jnp.float32
            )
            spread[pl.ds(i, comps_rows, stride=PITCH), :] = term
            return carry

        lax.fori_loop(0, size, one_pair, 0, unroll=32)

    def store_terms(lo, size, c, r0, spread):
        for l in range(levels):
            r = r0 + l
            block = spread[r * PITCH : r * PITCH + size, :].astype(jnp.bfloat16)
            terms[l // part, c, l % part, lo : lo + size, :] = block

    spans = [slice(c, c + 1) for c in range(comps)]
    fields = range(1, comps)

    def raw_copy(g, k, role, t):
        lo, size = (0, pairs) if k is None else (PIECES if g else WET_PIECES)[k]
        if t < 2:
            peer, data, mine = at(HOP[role], t), at(FAR[role], t), core
        else:
            peer, data, mine = twin, at(NEAR[role], other), 2
        return pltpu.make_async_remote_copy(
            src_ref=terms.at[data, spans[g], role % part, lo : lo + size],
            dst_ref=raw_r.at[role, mine, spans[g], lo : lo + size],
            send_sem=raw_ss,
            recv_sem=raw_rs.at[g, role // 2],
            device_id={"narrow": peer},
            device_id_type=MESH,
        )

    def send_raw(g, k, roles):
        for t in range(3):
            for role in roles:
                raw_copy(g, k, role, t).start()

    def wait_raw(g, roles):
        lo, hi = roles[0], roles[-1] + 1
        whole(raw_r.at[lo:hi, :, spans[g]], raw_ss, raw_rs.at[g, lo // 2]).wait_recv()

    first[2].wait()
    first[3].wait()
    level_ids = lax.broadcasted_iota(jnp.int32, (levels, lanes), 0)
    for s in range(own_tiles):
        wet = level_ids < depth_v[s : s + 1, :]
        wet_tiles[s] = jnp.where(wet, 1.0, 0.0).astype(jnp.bfloat16)
    for k, (lo, size) in enumerate(WET_PIECES):
        for b in range(lo // FETCH, (lo + size) // FETCH):
            counts_copy(b).wait()
        terms_of(lo, size, wet_tiles, wet_spread)
        store_terms(lo, size, 0, 0, wet_spread)
        send_raw(0, k, (0, 1))
        send_raw(0, k, (2, 3))

    whole(target_r.at[1:], target_ss, target_rs).wait_recv()
    for side, hop in enumerate((-1, 1)):
        for q, m in enumerate((at(hop, 0), at(hop, 1), twin, n)):
            row = target_r[m]
            for o in range(offsets):
                ids = o * TB_DEV + lax.broadcasted_iota(jnp.int32, (TB_DEV, pairs), 0)
                hit = jnp.where(ids == row, 1.0, 0.0).astype(jnp.bfloat16)
                select[side, o, :, q * pairs : (q + 1) * pairs] = hit

    own_field.wait()
    whole(field_r.at[1:], field_ss, field_rs).wait_recv()
    for m in range(narrow):
        for v in range(variables):
            for s in range(own_tiles):
                piece = field_r[m, v, :, s * lanes : (s + 1) * lanes]
                rows_f[s, v * levels + m * part : v * levels + (m + 1) * part, :] = piece.astype(jnp.float32)
    for s in range(own_tiles):
        wet = level_ids < depth_v[s : s + 1, :]
        for v in range(variables):
            rows = rows_f[s, v * levels : (v + 1) * levels, :]
            field_tiles[s, v * levels : (v + 1) * levels, :] = jnp.where(wet, rows, 0.0).astype(jnp.bfloat16)

    for k, (lo, size) in enumerate(PIECES):
        terms_of(lo, size, field_tiles, field_spread)
        for v in range(variables):
            store_terms(lo, size, v + 1, v * levels, field_spread)
        for g in fields:
            send_raw(g, k, (0, 1))

    def gathered(g, role):
        mine = at(NEAR[role], core)
        columns = []
        for c in range(spans[g].start, spans[g].stop):
            columns.append(
                jnp.concatenate([raw_r[role, t, c] for t in range(3)] + [terms[mine, c, role % part]], axis=0)
            )
        return jnp.concatenate(columns, axis=1) if len(columns) > 1 else columns[0]

    def add_up(role, o, received):
        side = 0 if HOP[role] == 1 else 1
        return jnp.dot(select[side, o], received, preferred_element_type=jnp.float32)

    def dense_copy(g, j, o, peer):
        return pltpu.make_async_remote_copy(
            src_ref=dense_s.at[j, o, spans[g]],
            dst_ref=dense_r.at[j, o, spans[g]],
            send_sem=dense_ss,
            recv_sem=dense_rs.at[g, o],
            device_id={"narrow": peer},
            device_id_type=MESH,
        )

    def relay(g, o, received):
        for role in (0, 1):
            total = add_up(role, o, received[role])
            for i, c in enumerate(range(spans[g].start, spans[g].stop)):
                dense_s[role, o, c] = total[:, i * lanes : (i + 1) * lanes].astype(jnp.bfloat16)

    def pass_on(g, o):
        for role in (0, 1):
            dense_copy(g, role, o, at(HOP[role], core)).start()

    def gather_own(g, offs):
        received = [gathered(g, role) for role in (2, 3)]
        for o in offs:
            for role in (2, 3):
                total = add_up(role, o, received[role - 2])
                for i, c in enumerate(range(spans[g].start, spans[g].stop)):
                    partial[o, c, role % part] = total[:, i * lanes : (i + 1) * lanes]

    def wide_copy(g, o, to):
        return pltpu.make_async_remote_copy(
            src_ref=sums.at[o, spans[g]],
            dst_ref=sums_r.at[o, spans[g]],
            send_sem=wide_ss,
            recv_sem=wide_rs.at[g],
            device_id={"wide": to},
            device_id_type=MESH,
        )

    def finish(g, o, leaves):
        whole(dense_r.at[:, o, spans[g]], dense_ss, dense_rs.at[g, o]).wait_recv()
        for c in range(spans[g].start, spans[g].stop):
            for j in range(part):
                total = partial[o, c, j] + dense_r[j, o, c].astype(jnp.float32)
                if leaves:
                    sums[o, c, j] = total.astype(jnp.bfloat16)
                else:
                    partial[o, c, j] = total
        if leaves:
            wide_copy(g, o, on_wide(o - REACH)).start()

    def relays(g, offs, received):
        for o in offs:
            relay(g, o, received)
            pass_on(g, o)

    rest = patient + [REACH]
    received = []
    for g in range(comps):
        wait_raw(g, (0, 1))
        received.append([gathered(g, role) for role in (0, 1)])
        relays(g, urgent, received[g])
        if g < variables:
            send_raw(g + 1, None, (2, 3))
        if g == 0:
            wait_raw(0, (2, 3))
            gather_own(0, urgent + rest)

    @pl.when(core == 1)
    def _():
        pl.semaphore_wait(barrier, 2 * len(shifts))
        pl.semaphore_signal(wide_in, inc=1, device_id={"narrow": twin}, device_id_type=MESH)

    @pl.when(core == 0)
    def _():
        pl.semaphore_wait(wide_in, 1)

    for o in urgent:
        finish(0, o, True)
    for g in range(comps):
        relays(g, rest, received[g])
    for g in fields:
        wait_raw(g, (2, 3))
        gather_own(g, urgent)
        for o in urgent:
            finish(g, o, True)
        gather_own(g, rest)
    for g in range(comps):
        for o in patient:
            finish(g, o, True)
    for g in range(comps):
        finish(g, REACH, False)

    own_part = own_cells * (narrow - 1)
    whole(field_v.at[:, :, :own_part], field_ss, field_rs).wait_send()
    whole(target_r.at[1:], target_ss, target_rs).wait_send()
    whole(terms.at[2:], raw_ss, raw_rs.at[0, 0]).wait_send()
    whole(dense_s, dense_ss, dense_rs.at[0, 0]).wait_send()

    def total_of(c):
        total = partial[REACH, c]
        for o in shifts:
            total = total + sums_r[o, c].astype(jnp.float32)
        return total

    whole(sums_r.at[1:, spans[0]], wide_ss, wide_rs.at[0]).wait_recv()
    wet_total = total_of(0)
    covered = wet_total > WET_LIMIT
    safe = jnp.where(covered, wet_total, 1.0)
    for v in range(variables):
        whole(sums_r.at[1:, spans[v + 1]], wide_ss, wide_rs.at[v + 1]).wait_recv()
        result = jnp.where(covered, total_of(v + 1) / safe, 0.0)
        for j in range(part):
            paired[v, pl.ds(j, TB_DEV, stride=part), :] = result[j]
        for t in range(TB_DEV):
            out_ref[v, :, t * lanes : (t + 1) * lanes] = paired[v, t * part : (t + 1) * part, :].astype(out_ref.dtype)

    whole(sums.at[1:], wide_ss, wide_rs.at[0]).wait_send()


def per_device(wide, narrow, src_field, src_depth, packed_counts, pair_source, pair_home, pair_count):
    variables, part, _ = src_field.shape
    pairs, _, lanes = packed_counts.shape
    own_tiles = src_depth.shape[0] // lanes
    levels = narrow * part
    comps = variables + 1
    offsets = 2 * REACH + 1
    dma = pltpu.SemaphoreType.DMA
    bf16, f32, i32 = jnp.bfloat16, jnp.float32, jnp.int32
    in_hbm = pl.BlockSpec(memory_space=pltpu.HBM)
    return pl.pallas_call(
        functools.partial(kernel, wide, narrow),
        out_shape=pltpu.VMEM((variables, part, TB_DEV * lanes), bf16),
        in_specs=[in_hbm] * 5 + [pl.BlockSpec(memory_space=pltpu.SMEM)],
        out_specs=pl.BlockSpec(memory_space=pltpu.VMEM),
        scratch_shapes=[
            pltpu.VMEM(src_field.shape, bf16),
            pltpu.VMEM((own_tiles, lanes), i32),
            pltpu.VMEM(packed_counts.shape, i32),
            pltpu.VMEM((1, pairs), i32),
            pltpu.SMEM((pairs,), i32),
            pltpu.VMEM((1, 1, pairs), i32),
            pltpu.VMEM((narrow, 1, pairs), i32),
            pltpu.VMEM((narrow, variables, part, own_tiles * lanes), bf16),
            pltpu.VMEM((own_tiles, variables * levels, lanes), f32),
            pltpu.VMEM((own_tiles, levels, lanes), bf16),
            pltpu.VMEM((own_tiles, variables * levels, lanes), bf16),
            pltpu.VMEM((levels * PITCH, lanes), f32),
            pltpu.VMEM((variables * levels * PITCH, lanes), f32),
            pltpu.VMEM((variables, TB_DEV * part, lanes), f32),
            pltpu.VMEM((narrow, comps, part, pairs, lanes), bf16),
            pltpu.VMEM((4, 3, comps, pairs, lanes), bf16),
            pltpu.VMEM((2, offsets, TB_DEV, 4 * pairs), bf16),
            pltpu.VMEM((part, offsets, comps, TB_DEV, lanes), bf16),
            pltpu.VMEM((part, offsets, comps, TB_DEV, lanes), bf16),
            pltpu.VMEM((offsets, comps, part, TB_DEV, lanes), f32),
            pltpu.VMEM((offsets, comps, part, TB_DEV, lanes), bf16),
            pltpu.VMEM((offsets, comps, part, TB_DEV, lanes), bf16),
            pltpu.SemaphoreType.REGULAR,
            pltpu.SemaphoreType.REGULAR,
            dma((4,)),
            dma((pairs // FETCH,)),
            dma(()),
            dma(()),
            dma(()),
            dma(()),
            dma(()),
            dma(()),
            dma((comps, 2)),
            dma(()),
            dma((comps, offsets)),
            dma(()),
            dma((comps,)),
        ],
        compiler_params=pltpu.CompilerParams(collective_id=0, has_side_effects=True),
    )(
        src_field,
        src_depth.reshape(own_tiles, lanes),
        packed_counts,
        pair_source,
        pair_home.reshape(1, pairs),
        pair_count,
    )


def solution(mesh):
    both = ("wide", "narrow")
    return jax.shard_map(
        functools.partial(per_device, mesh.shape["wide"], mesh.shape["narrow"]),
        mesh=mesh,
        in_specs=(P(None, "narrow", "wide"), P(both), P(both, None, None), P(both), P(both), P(both)),
        out_specs=P(None, "narrow", "wide"),
        check_vma=False,
    )
```

```python
import functools

import jax
import jax.numpy as jnp
from jax import lax
from jax.experimental import pallas as pl
from jax.experimental.pallas import tpu as pltpu
from jax.sharding import PartitionSpec as P

DENOM = 256
REACH = 2
TB_DEV = 64
WET_LIMIT = 0.001
FETCH = 32
WET_PIECES = ((0, 64), (64, 64))
PIECES = ((0, 32), (32, 32), (64, 32), (96, 32))
PITCH = 72
MESH = pl.DeviceIdType.MESH

HOP = (1, -1, -1, 1)
FAR = (2, -2, -1, 1)
NEAR = (1, -1, 0, 0)


def kernel(
    wide,
    narrow,
    field_in,
    depth_in,
    counts_in,
    source_in,
    home_in,
    live_in,
    out_ref,
    field_v,
    depth_v,
    counts_v,
    home_v,
    source_s,
    target_v,
    target_r,
    field_r,
    rows_f,
    wet_tiles,
    field_tiles,
    wet_spread,
    field_spread,
    paired,
    terms,
    raw_r,
    select,
    dense_s,
    dense_r,
    partial,
    sums,
    sums_r,
    group_in,
    wide_in,
    local_sem,
    counts_sem,
    self_sem,
    field_ss,
    field_rs,
    target_ss,
    target_rs,
    raw_ss,
    raw_rs,
    dense_ss,
    dense_rs,
    wide_ss,
    wide_rs,
):
    w = lax.axis_index("wide")
    n = lax.axis_index("narrow")
    pairs, half, lanes = counts_v.shape
    own_tiles = wet_tiles.shape[0]
    own_cells = own_tiles * lanes
    variables, part = field_v.shape[0], field_v.shape[1]
    levels = narrow * part
    comps = variables + 1
    offsets = 2 * REACH + 1
    shifts = [o for o in range(offsets) if o != REACH]
    chips = narrow // 2
    core = lax.rem(n, 2)
    chip = n // 2
    other = 1 - core
    twin = 2 * chip + other

    column = lax.rem(w, 8)
    middle = (column // 4) * (1 - lax.rem(column // 2, 2))
    edge = (column // 4) * lax.rem(column // 2, 2) * lax.rem(column, 2)
    urgent = [4 - 4 * middle - edge, 3 - 2 * middle + edge]
    patient = [4 * middle, 1 + 2 * middle]

    def at(hop, c):
        return lax.rem(chip + hop + chips, chips) * 2 + c

    def on_narrow(step):
        return lax.rem(n + step, narrow)

    def on_wide(shift):
        return lax.rem(w + shift + wide, wide)

    def whole(ref, send_sem, recv_sem):
        return pltpu.make_async_remote_copy(
            src_ref=ref,
            dst_ref=ref,
            send_sem=send_sem,
            recv_sem=recv_sem,
            device_id={"narrow": twin},
            device_id_type=MESH,
        )

    first = [
        pltpu.make_async_copy(field_in, field_v, local_sem.at[0]),
        pltpu.make_async_copy(home_in, home_v, local_sem.at[1]),
        pltpu.make_async_copy(depth_in, depth_v, local_sem.at[2]),
        pltpu.make_async_copy(source_in, source_s, local_sem.at[3]),
    ]
    for copy in first:
        copy.start()

    def counts_copy(b):
        rows = pl.ds(b * FETCH, FETCH)
        return pltpu.make_async_copy(counts_in.at[rows], counts_v.at[rows], counts_sem.at[b])

    for b in range(pairs // FETCH):
        counts_copy(b).start()

    barrier = pltpu.get_barrier_semaphore()
    for hop in range(1, chips):
        pl.semaphore_signal(barrier, inc=1, device_id={"narrow": at(hop, 0)}, device_id_type=MESH)
    for o in shifts:
        pl.semaphore_signal(
            barrier, inc=1, device_id={"wide": on_wide(o - REACH), "narrow": at(0, 1)}, device_id_type=MESH
        )

    @pl.when(core == 1)
    def _():
        pl.semaphore_signal(barrier, inc=1, device_id={"narrow": twin}, device_id_type=MESH)

    first[1].wait()
    home = home_v[...]
    slot = lax.broadcasted_iota(jnp.int32, home.shape, 1)
    offset = lax.rem(home // TB_DEV - w + REACH + wide, wide)
    target = jnp.where(slot < live_in[0], offset * TB_DEV + lax.rem(home, TB_DEV), -1)
    target_v[0] = target
    target_r[n] = target
    first[0].wait()

    @pl.when(core == 0)
    def _():
        pl.semaphore_wait(barrier, narrow - 1)
        pl.semaphore_signal(group_in, inc=1, device_id={"narrow": twin}, device_id_type=MESH)

    @pl.when(core == 1)
    def _():
        pl.semaphore_wait(group_in, 1)

    order = [2, 6, 4, 3, 7, 5, 1]

    def field_copy(step, peer, to):
        cells = pl.ds(pl.multiple_of(peer * own_cells, own_cells), own_cells)
        return pltpu.make_async_remote_copy(
            src_ref=field_v.at[:, :, cells],
            dst_ref=field_r.at[to],
            send_sem=field_ss,
            recv_sem=field_rs,
            device_id={"narrow": peer},
            device_id_type=MESH,
        )

    def target_copy(step, peer, to):
        return pltpu.make_async_remote_copy(
            src_ref=target_v,
            dst_ref=target_r.at[pl.ds(to, 1)],
            send_sem=target_ss,
            recv_sem=target_rs,
            device_id={"narrow": peer},
            device_id_type=MESH,
        )

    for step in order:
        target_copy(step, on_narrow(step), n).start()
    for step in order:
        field_copy(step, on_narrow(step), n).start()
    own_span = pl.ds(pl.multiple_of(n * own_cells, own_cells), own_cells)
    own_field = pltpu.make_async_copy(field_v.at[:, :, own_span], field_r.at[n], self_sem)
    own_field.start()

    def terms_of(lo, size, stored, spread):
        comps_rows = stored.shape[1]

        def one_pair(i, carry):
            p = lo + i
            words = counts_v[p]
            low = (words & 65535).astype(jnp.float32) * (1.0 / DENOM)
            high = lax.shift_right_logical(words, 16).astype(jnp.float32) * (1.0 / DENOM)
            weight = jnp.concatenate([low.astype(jnp.bfloat16), high.astype(jnp.bfloat16)], axis=0)
            term = lax.dot_general(
                stored[source_s[p]], weight, (((1,), (1,)), ((), ())), preferred_element_type=jnp.float32
            )
            spread[pl.ds(i, comps_rows, stride=PITCH), :] = term
            return carry

        lax.fori_loop(0, size, one_pair, 0, unroll=32)

    def store_terms(lo, size, c, r0, spread):
        for l in range(levels):
            r = r0 + l
            block = spread[r * PITCH : r * PITCH + size, :].astype(jnp.bfloat16)
            terms[l // part, c, l % part, lo : lo + size, :] = block

    spans = [slice(c, c + 1) for c in range(comps)]
    fields = range(1, comps)

    def raw_copy(g, k, role, t):
        lo, size = (0, pairs) if k is None else (PIECES if g else WET_PIECES)[k]
        if t < 2:
            peer, data, mine = at(HOP[role], t), at(FAR[role], t), core
        else:
            peer, data, mine = twin, at(NEAR[role], other), 2
        return pltpu.make_async_remote_copy(
            src_ref=terms.at[data, spans[g], role % part, lo : lo + size],
            dst_ref=raw_r.at[role, mine, spans[g], lo : lo + size],
            send_sem=raw_ss,
            recv_sem=raw_rs.at[g, role // 2],
            device_id={"narrow": peer},
            device_id_type=MESH,
        )

    def send_raw(g, k, roles):
        for t in range(3):
            for role in roles:
                raw_copy(g, k, role, t).start()

    def wait_raw(g, roles):
        lo, hi = roles[0], roles[-1] + 1
        whole(raw_r.at[lo:hi, :, spans[g]], raw_ss, raw_rs.at[g, lo // 2]).wait_recv()

    first[2].wait()
    first[3].wait()
    level_ids = lax.broadcasted_iota(jnp.int32, (levels, lanes), 0)
    for s in range(own_tiles):
        wet = level_ids < depth_v[s : s + 1, :]
        wet_tiles[s] = jnp.where(wet, 1.0, 0.0).astype(jnp.bfloat16)
    for k, (lo, size) in enumerate(WET_PIECES):
        for b in range(lo // FETCH, (lo + size) // FETCH):
            counts_copy(b).wait()
        terms_of(lo, size, wet_tiles, wet_spread)
        store_terms(lo, size, 0, 0, wet_spread)
        send_raw(0, k, (0, 1))
        send_raw(0, k, (2, 3))

    whole(target_r.at[1:], target_ss, target_rs).wait_recv()
    for side, hop in enumerate((-1, 1)):
        for q, m in enumerate((at(hop, 0), at(hop, 1), twin, n)):
            row = target_r[m]
            for o in range(offsets):
                ids = o * TB_DEV + lax.broadcasted_iota(jnp.int32, (TB_DEV, pairs), 0)
                hit = jnp.where(ids == row, 1.0, 0.0).astype(jnp.bfloat16)
                select[side, o, :, q * pairs : (q + 1) * pairs] = hit

    own_field.wait()
    whole(field_r.at[1:], field_ss, field_rs).wait_recv()
    for m in range(narrow):
        for v in range(variables):
            for s in range(own_tiles):
                piece = field_r[m, v, :, s * lanes : (s + 1) * lanes]
                rows_f[s, v * levels + m * part : v * levels + (m + 1) * part, :] = piece.astype(jnp.float32)
    for s in range(own_tiles):
        wet = level_ids < depth_v[s : s + 1, :]
        for v in range(variables):
            rows = rows_f[s, v * levels : (v + 1) * levels, :]
            field_tiles[s, v * levels : (v + 1) * levels, :] = jnp.where(wet, rows, 0.0).astype(jnp.bfloat16)

    for k, (lo, size) in enumerate(PIECES):
        terms_of(lo, size, field_tiles, field_spread)
        for v in range(variables):
            store_terms(lo, size, v + 1, v * levels, field_spread)
        for g in fields:
            send_raw(g, k, (0, 1))

    def gathered(g, role):
        mine = at(NEAR[role], core)
        columns = []
        for c in range(spans[g].start, spans[g].stop):
            columns.append(
                jnp.concatenate([raw_r[role, t, c] for t in range(3)] + [terms[mine, c, role % part]], axis=0)
            )
        return jnp.concatenate(columns, axis=1) if len(columns) > 1 else columns[0]

    def add_up(role, o, received):
        side = 0 if HOP[role] == 1 else 1
        return jnp.dot(select[side, o], received, preferred_element_type=jnp.float32)

    def dense_copy(g, j, o, peer):
        return pltpu.make_async_remote_copy(
            src_ref=dense_s.at[j, o, spans[g]],
            dst_ref=dense_r.at[j, o, spans[g]],
            send_sem=dense_ss,
            recv_sem=dense_rs.at[g, o],
            device_id={"narrow": peer},
            device_id_type=MESH,
        )

    def relay(g, o, received):
        for role in (0, 1):
            total = add_up(role, o, received[role])
            for i, c in enumerate(range(spans[g].start, spans[g].stop)):
                dense_s[role, o, c] = total[:, i * lanes : (i + 1) * lanes].astype(jnp.bfloat16)

    def pass_on(g, o):
        for role in (0, 1):
            dense_copy(g, role, o, at(HOP[role], core)).start()

    def gather_own(g, offs):
        received = [gathered(g, role) for role in (2, 3)]
        for o in offs:
            for role in (2, 3):
                total = add_up(role, o, received[role - 2])
                for i, c in enumerate(range(spans[g].start, spans[g].stop)):
                    partial[o, c, role % part] = total[:, i * lanes : (i + 1) * lanes]

    def wide_copy(g, o, to):
        return pltpu.make_async_remote_copy(
            src_ref=sums.at[o, spans[g]],
            dst_ref=sums_r.at[o, spans[g]],
            send_sem=wide_ss,
            recv_sem=wide_rs.at[g],
            device_id={"wide": to},
            device_id_type=MESH,
        )

    def finish(g, o, leaves):
        whole(dense_r.at[:, o, spans[g]], dense_ss, dense_rs.at[g, o]).wait_recv()
        for c in range(spans[g].start, spans[g].stop):
            for j in range(part):
                total = partial[o, c, j] + dense_r[j, o, c].astype(jnp.float32)
                if leaves:
                    sums[o, c, j] = total.astype(jnp.bfloat16)
                else:
                    partial[o, c, j] = total
        if leaves:
            wide_copy(g, o, on_wide(o - REACH)).start()

    def relays(g, offs, received):
        for o in offs:
            relay(g, o, received)
            pass_on(g, o)

    rest = patient + [REACH]
    received = []
    for g in range(comps):
        wait_raw(g, (0, 1))
        received.append([gathered(g, role) for role in (0, 1)])
        relays(g, urgent, received[g])
        if g == 0:
            for later in fields:
                send_raw(later, None, (2, 3))
            wait_raw(0, (2, 3))
            gather_own(0, urgent + rest)

    @pl.when(core == 1)
    def _():
        pl.semaphore_wait(barrier, 2 * len(shifts))
        pl.semaphore_signal(wide_in, inc=1, device_id={"narrow": twin}, device_id_type=MESH)

    @pl.when(core == 0)
    def _():
        pl.semaphore_wait(wide_in, 1)

    for o in urgent:
        finish(0, o, True)
    for g in range(comps):
        relays(g, rest, received[g])
    for g in fields:
        wait_raw(g, (2, 3))
        gather_own(g, urgent)
        for o in urgent:
            finish(g, o, True)
        gather_own(g, rest)
    for g in range(comps):
        for o in patient:
            finish(g, o, True)
    for g in range(comps):
        finish(g, REACH, False)

    own_part = own_cells * (narrow - 1)
    whole(field_v.at[:, :, :own_part], field_ss, field_rs).wait_send()
    whole(target_r.at[1:], target_ss, target_rs).wait_send()
    whole(terms.at[2:], raw_ss, raw_rs.at[0, 0]).wait_send()
    whole(dense_s, dense_ss, dense_rs.at[0, 0]).wait_send()

    def total_of(c):
        total = partial[REACH, c]
        for o in shifts:
            total = total + sums_r[o, c].astype(jnp.float32)
        return total

    whole(sums_r.at[1:, spans[0]], wide_ss, wide_rs.at[0]).wait_recv()
    wet_total = total_of(0)
    covered = wet_total > WET_LIMIT
    safe = jnp.where(covered, wet_total, 1.0)
    for v in range(variables):
        whole(sums_r.at[1:, spans[v + 1]], wide_ss, wide_rs.at[v + 1]).wait_recv()
        result = jnp.where(covered, total_of(v + 1) / safe, 0.0)
        for j in range(part):
            paired[v, pl.ds(j, TB_DEV, stride=part), :] = result[j]
        for t in range(TB_DEV):
            out_ref[v, :, t * lanes : (t + 1) * lanes] = paired[v, t * part : (t + 1) * part, :].astype(out_ref.dtype)

    whole(sums.at[1:], wide_ss, wide_rs.at[0]).wait_send()


def per_device(wide, narrow, src_field, src_depth, packed_counts, pair_source, pair_home, pair_count):
    variables, part, _ = src_field.shape
    pairs, _, lanes = packed_counts.shape
    own_tiles = src_depth.shape[0] // lanes
    levels = narrow * part
    comps = variables + 1
    offsets = 2 * REACH + 1
    dma = pltpu.SemaphoreType.DMA
    bf16, f32, i32 = jnp.bfloat16, jnp.float32, jnp.int32
    in_hbm = pl.BlockSpec(memory_space=pltpu.HBM)
    return pl.pallas_call(
        functools.partial(kernel, wide, narrow),
        out_shape=pltpu.VMEM((variables, part, TB_DEV * lanes), bf16),
        in_specs=[in_hbm] * 5 + [pl.BlockSpec(memory_space=pltpu.SMEM)],
        out_specs=pl.BlockSpec(memory_space=pltpu.VMEM),
        scratch_shapes=[
            pltpu.VMEM(src_field.shape, bf16),
            pltpu.VMEM((own_tiles, lanes), i32),
            pltpu.VMEM(packed_counts.shape, i32),
            pltpu.VMEM((1, pairs), i32),
            pltpu.SMEM((pairs,), i32),
            pltpu.VMEM((1, 1, pairs), i32),
            pltpu.VMEM((narrow, 1, pairs), i32),
            pltpu.VMEM((narrow, variables, part, own_tiles * lanes), bf16),
            pltpu.VMEM((own_tiles, variables * levels, lanes), f32),
            pltpu.VMEM((own_tiles, levels, lanes), bf16),
            pltpu.VMEM((own_tiles, variables * levels, lanes), bf16),
            pltpu.VMEM((levels * PITCH, lanes), f32),
            pltpu.VMEM((variables * levels * PITCH, lanes), f32),
            pltpu.VMEM((variables, TB_DEV * part, lanes), f32),
            pltpu.VMEM((narrow, comps, part, pairs, lanes), bf16),
            pltpu.VMEM((4, 3, comps, pairs, lanes), bf16),
            pltpu.VMEM((2, offsets, TB_DEV, 4 * pairs), bf16),
            pltpu.VMEM((part, offsets, comps, TB_DEV, lanes), bf16),
            pltpu.VMEM((part, offsets, comps, TB_DEV, lanes), bf16),
            pltpu.VMEM((offsets, comps, part, TB_DEV, lanes), f32),
            pltpu.VMEM((offsets, comps, part, TB_DEV, lanes), bf16),
            pltpu.VMEM((offsets, comps, part, TB_DEV, lanes), bf16),
            pltpu.SemaphoreType.REGULAR,
            pltpu.SemaphoreType.REGULAR,
            dma((4,)),
            dma((pairs // FETCH,)),
            dma(()),
            dma(()),
            dma(()),
            dma(()),
            dma(()),
            dma(()),
            dma((comps, 2)),
            dma(()),
            dma((comps, offsets)),
            dma(()),
            dma((comps,)),
        ],
        compiler_params=pltpu.CompilerParams(collective_id=0, has_side_effects=True),
    )(
        src_field,
        src_depth.reshape(own_tiles, lanes),
        packed_counts,
        pair_source,
        pair_home.reshape(1, pairs),
        pair_count,
    )


def solution(mesh):
    both = ("wide", "narrow")
    return jax.shard_map(
        functools.partial(per_device, mesh.shape["wide"], mesh.shape["narrow"]),
        mesh=mesh,
        in_specs=(P(None, "narrow", "wide"), P(both), P(both, None, None), P(both), P(both), P(both)),
        out_specs=P(None, "narrow", "wide"),
        check_vma=False,
    )
```
